128 devices in a mesh: dp: 1, tp: 16 (over z, y), cp: 8 (over x, core).
Axes of the slice: x: 4, y: 4, z: 4, core: 2. Of those that a mesh axis runs over, the one named last changes fastest.
Arguments:
- x_in: bfloat16 [8192, 4096], P(('dp', 'cp', 'tp'))
- w_query: bfloat16 [4096, 32, 128], P(None, 'tp')
- w_key: bfloat16 [4096, 32, 128], P(None, 'tp')
- w_value: bfloat16 [4096, 32, 128], P(None, 'tp')
- w_out: bfloat16 [32, 128, 4096], P('tp')
- d_out: bfloat16 [8192, 4096], P(('dp', 'cp', 'tp'))
Outputs:
- output 1: bfloat16 [8192, 4096], P(('dp', 'cp', 'tp'))
- output 2: bfloat16 [8192, 4096], P(('dp', 'cp', 'tp'))
- output 3: bfloat16 [8, 4096, 32, 128], P(('dp', 'cp'), None, 'tp')
- output 4: bfloat16 [8, 4096, 32, 128], P(('dp', 'cp'), None, 'tp')
- output 5: bfloat16 [8, 4096, 32, 128], P(('dp', 'cp'), None, 'tp')
- output 6: bfloat16 [8, 32, 128, 4096], P(('dp', 'cp'), 'tp')
All inputs are finite; a program needn't handle non-finite values.
Results may differ from the reference program's by a relative error of at most 0.00935223.
Values are sent between devices in bfloat16 or wider.
A program may use at most 1 GiB of HBM per device.

```python
import math
import jax
import jax.numpy as jnp
from jax import lax

MODEL_DIM = 4096
NUM_HEADS = 32
NUM_KV_HEADS = 32
HEAD_DIM = 128
SEQ_LEN = 8192
SEQ_SHARDS = 8
QUERY_BLOCK = 32


def setup_inputs(seed: int = 0, part: int = 0) -> dict:
    shared_keys = jax.random.split(jax.random.key(seed), 4)
    part_keys = jax.random.split(jax.random.fold_in(jax.random.key(seed), part), 2)
    logit_gain = 1.6
    in_scale = 1.0 / math.sqrt(MODEL_DIM)
    x_in = jax.random.normal(part_keys[0], (SEQ_LEN, MODEL_DIM), jnp.float32)
    w_query = jax.random.normal(shared_keys[0], (MODEL_DIM, NUM_HEADS, HEAD_DIM), jnp.float32) * (logit_gain * in_scale)
    w_key = jax.random.normal(shared_keys[1], (MODEL_DIM, NUM_KV_HEADS, HEAD_DIM), jnp.float32) * (logit_gain * in_scale)
    w_value = jax.random.normal(shared_keys[2], (MODEL_DIM, NUM_KV_HEADS, HEAD_DIM), jnp.float32) * in_scale
    w_out = jax.random.normal(shared_keys[3], (NUM_HEADS, HEAD_DIM, MODEL_DIM), jnp.float32) / math.sqrt(NUM_HEADS * HEAD_DIM)
    d_out = jax.random.normal(part_keys[1], (SEQ_LEN, MODEL_DIM), jnp.float32)
    return {"x_in": x_in.astype(jnp.bfloat16), "w_query": w_query.astype(jnp.bfloat16), "w_key": w_key.astype(jnp.bfloat16), "w_value": w_value.astype(jnp.bfloat16), "w_out": w_out.astype(jnp.bfloat16), "d_out": d_out.astype(jnp.bfloat16)}


def stored_positions():
    half_rows = SEQ_LEN // (2 * SEQ_SHARDS)
    row_ids = jnp.arange(SEQ_LEN, dtype=jnp.int32)
    shard_id = row_ids // (2 * half_rows)
    within = row_ids % (2 * half_rows)
    return jnp.where(within < half_rows, shard_id * half_rows + within, (2 * SEQ_SHARDS - 1 - shard_id) * half_rows + within - half_rows)


def reference(x_in, w_query, w_key, w_value, w_out, d_out):
    groups = NUM_HEADS // NUM_KV_HEADS
    attn_scale = 1.0 / math.sqrt(HEAD_DIM)
    n_blocks = SEQ_LEN // QUERY_BLOCK
    shard_rows = SEQ_LEN // SEQ_SHARDS
    q_cols = NUM_HEADS * HEAD_DIM
    kv_cols = NUM_KV_HEADS * HEAD_DIM
    wq_flat = w_query.reshape(MODEL_DIM, q_cols)
    wk_flat = w_key.reshape(MODEL_DIM, kv_cols)
    wv_flat = w_value.reshape(MODEL_DIM, kv_cols)
    wo_flat = w_out.reshape(q_cols, MODEL_DIM)
    q_flat = jnp.dot(x_in, wq_flat, preferred_element_type=jnp.float32).astype(jnp.bfloat16)
    k_flat = jnp.dot(x_in, wk_flat, preferred_element_type=jnp.float32).astype(jnp.bfloat16)
    v_flat = jnp.dot(x_in, wv_flat, preferred_element_type=jnp.float32).astype(jnp.bfloat16)
    positions = stored_positions()
    k_heads = k_flat.reshape(SEQ_LEN, NUM_KV_HEADS, HEAD_DIM).astype(jnp.float32)
    v_heads = v_flat.reshape(SEQ_LEN, NUM_KV_HEADS, HEAD_DIM).astype(jnp.float32)
    q_blocks = q_flat.reshape(n_blocks, QUERY_BLOCK, NUM_KV_HEADS, groups, HEAD_DIM)
    pos_blocks = positions.reshape(n_blocks, QUERY_BLOCK)

    def block_scores(q_blk, pos_blk):
        scores = jnp.einsum("qhgd,khd->qhgk", q_blk.astype(jnp.float32), k_heads) * attn_scale
        visible = pos_blk[:, None, None, None] >= positions[None, None, None, :]
        return jnp.where(visible, scores, -jnp.inf)

    def forward_block(block_in):
        q_blk, pos_blk = block_in
        scores = block_scores(q_blk, pos_blk)
        row_max = jnp.max(scores, axis=-1)
        prob_mat = jnp.exp(scores - row_max[..., None])
        row_sum = jnp.sum(prob_mat, axis=-1)
        pv_sum = jnp.einsum("qhgk,khd->qhgd", prob_mat.astype(jnp.bfloat16).astype(jnp.float32), v_heads)
        out_blk = (pv_sum / row_sum[..., None]).astype(jnp.bfloat16)
        return out_blk, row_max + jnp.log(row_sum)

    o_blocks, lse_blocks = lax.map(forward_block, (q_blocks, pos_blocks))
    o_flat = o_blocks.reshape(SEQ_LEN, q_cols)
    y_out = jnp.dot(o_flat, wo_flat, preferred_element_type=jnp.float32).astype(jnp.bfloat16)

    do_flat = jnp.dot(d_out, wo_flat.T, preferred_element_type=jnp.float32).astype(jnp.bfloat16)
    do_blocks = do_flat.reshape(n_blocks, QUERY_BLOCK, NUM_KV_HEADS, groups, HEAD_DIM)
    dot_blocks = jnp.sum(do_blocks.astype(jnp.float32) * o_blocks.astype(jnp.float32), axis=-1)

    def backward_block(grad_carry, block_in):
        dk_acc, dv_acc = grad_carry
        q_blk, pos_blk, lse_blk, do_blk, dot_blk = block_in
        scores = block_scores(q_blk, pos_blk)
        prob_mat = jnp.exp(scores - lse_blk[..., None])
        do_wide = do_blk.astype(jnp.float32)
        d_probs = jnp.einsum("qhgd,khd->qhgk", do_wide, v_heads)
        d_scores = (prob_mat * (d_probs - dot_blk[..., None])).astype(jnp.bfloat16).astype(jnp.float32)
        dv_acc = dv_acc + jnp.einsum("qhgk,qhgd->khd", prob_mat.astype(jnp.bfloat16).astype(jnp.float32), do_wide)
        dk_acc = dk_acc + jnp.einsum("qhgk,qhgd->khd", d_scores, q_blk.astype(jnp.float32)) * attn_scale
        dq_blk = jnp.einsum("qhgk,khd->qhgd", d_scores, k_heads) * attn_scale
        return (dk_acc, dv_acc), dq_blk.astype(jnp.bfloat16)

    zero_kv = jnp.zeros((SEQ_LEN, NUM_KV_HEADS, HEAD_DIM), jnp.float32)
    grad_kv, dq_blocks = lax.scan(backward_block, (zero_kv, zero_kv), (q_blocks, pos_blocks, lse_blocks, do_blocks, dot_blocks))
    dq_flat = dq_blocks.reshape(SEQ_LEN, q_cols)
    dk_flat = grad_kv[0].astype(jnp.bfloat16).reshape(SEQ_LEN, kv_cols)
    dv_flat = grad_kv[1].astype(jnp.bfloat16).reshape(SEQ_LEN, kv_cols)
    dx_sum = (jnp.dot(dq_flat, wq_flat.T, preferred_element_type=jnp.float32)
              + jnp.dot(dk_flat, wk_flat.T, preferred_element_type=jnp.float32)
              + jnp.dot(dv_flat, wv_flat.T, preferred_element_type=jnp.float32))
    grad_x = dx_sum.astype(jnp.bfloat16)
    x_shards = x_in.reshape(SEQ_SHARDS, shard_rows, MODEL_DIM).astype(jnp.float32)
    grad_wq = jnp.einsum("rsm,rsc->rmc", x_shards, dq_flat.reshape(SEQ_SHARDS, shard_rows, q_cols).astype(jnp.float32)).astype(jnp.bfloat16).reshape(SEQ_SHARDS, MODEL_DIM, NUM_HEADS, HEAD_DIM)
    grad_wk = jnp.einsum("rsm,rsc->rmc", x_shards, dk_flat.reshape(SEQ_SHARDS, shard_rows, kv_cols).astype(jnp.float32)).astype(jnp.bfloat16).reshape(SEQ_SHARDS, MODEL_DIM, NUM_KV_HEADS, HEAD_DIM)
    grad_wv = jnp.einsum("rsm,rsc->rmc", x_shards, dv_flat.reshape(SEQ_SHARDS, shard_rows, kv_cols).astype(jnp.float32)).astype(jnp.bfloat16).reshape(SEQ_SHARDS, MODEL_DIM, NUM_KV_HEADS, HEAD_DIM)
    grad_wo = jnp.einsum("rsc,rsm->rcm", o_flat.reshape(SEQ_SHARDS, shard_rows, q_cols).astype(jnp.float32), d_out.reshape(SEQ_SHARDS, shard_rows, MODEL_DIM).astype(jnp.float32)).astype(jnp.bfloat16).reshape(SEQ_SHARDS, NUM_HEADS, HEAD_DIM, MODEL_DIM)
    return y_out, grad_x, grad_wq, grad_wk, grad_wv, grad_wo
```

```python
import functools
import math

import jax
import jax.numpy as jnp
from jax import lax
from jax.experimental import pallas as pl
from jax.experimental.pallas import tpu as pltpu
from jax.sharding import PartitionSpec as P

ROW_SPEC = P(("dp", "cp", "tp"), None)
HEAD_SPEC = P(None, "tp", None)
OUT_W_SPEC = P("tp", None, None)
GRAD_SPEC = P(("dp", "cp"), None, "tp", None)
GRAD_OUT_SPEC = P(("dp", "cp"), "tp", None, None)
COLS_CONTRACT = (((1,), (1,)), ((), ()))
ROWS_CONTRACT = (((0,), (0,)), ((), ()))
VMEM_LIMIT = 58 * 1024 * 1024
F32 = jnp.float32
BF16 = jnp.bfloat16


def dot_t(lhs, rhs):
    return lax.dot_general(lhs, rhs, COLS_CONTRACT, preferred_element_type=F32)


def dot_n(lhs, rhs):
    return jnp.dot(lhs, rhs, preferred_element_type=F32)


def block_slot(pos_blk, n_sh):
    return jnp.where(pos_blk < n_sh, 2 * pos_blk, 2 * (2 * n_sh - 1 - pos_blk) + 1)


def shard_pieces(arr, n_sh):
    n_x = n_sh // 2
    ids = [(xi, ci) for xi in range(n_x) for ci in range(2)]
    plus = [(2 * xi + ci, 2 * ((xi + 1) % n_x) + ci) for xi, ci in ids]
    minus = [(2 * xi + ci, 2 * ((xi - 1) % n_x) + ci) for xi, ci in ids]
    swap = [(2 * xi + ci, 2 * xi + 1 - ci) for xi, ci in ids]
    from_prev = lax.ppermute(arr, "cp", plus)
    from_next = lax.ppermute(arr, "cp", minus)
    far_lo = lax.ppermute(from_prev[:1], "cp", plus)
    far_hi = lax.ppermute(from_next[1:], "cp", minus)
    pieces = [(arr, 0, 0, None), (from_prev, n_x - 1, 0, None), (from_next, 1, 0, None), (far_lo, 2, 0, 0), (far_hi, 2, 0, 1)]
    others = [(lax.ppermute(piece, "cp", swap), dx, 1, half) for piece, dx, _, half in pieces]
    return pieces + others


def load_pieces(refs, meta, buf, sems, rank, n_sh):
    n_x = n_sh // 2
    copies = []
    for idx, (ref, (dx, dc, half)) in enumerate(zip(refs, meta)):
        shard = 2 * lax.rem(rank // 2 + dx, n_x) + lax.rem(rank + dc, 2)
        start = 2 * shard + (0 if half is None else half)
        copy = pltpu.make_async_copy(ref, buf.at[pl.ds(start, ref.shape[0])], sems.at[idx])
        copy.start()
        copies.append(copy)
    return copies


def causal_mask(rows, cols, transposed=False):
    row_ids = lax.broadcasted_iota(jnp.int32, (rows, cols), 0)
    col_ids = lax.broadcasted_iota(jnp.int32, (rows, cols), 1)
    return col_ids >= row_ids if transposed else row_ids >= col_ids


def forward_kernel(n_sh, heads, dim, meta, rank_ref, q_ref, *rest):
    n_p = len(meta)
    kv_refs = rest[:n_p]
    o_ref, lse_ref, kv_buf, m_ref, l_ref, acc_ref, sems = rest[n_p:]
    rank = rank_ref[0]
    width = heads * dim
    half_rows = q_ref.shape[1]
    log2e_scale = math.log2(math.e) * dim ** -0.5
    copies = load_pieces(kv_refs, meta, kv_buf, sems, rank, n_sh)
    for copy in copies:
        copy.wait()
    for half in range(2):
        for h in range(heads):
            cols = slice(h * dim, (h + 1) * dim)
            vcols = slice(width + h * dim, width + (h + 1) * dim)
            k_blk = kv_buf[2 * rank + half, :, cols]
            v_blk = kv_buf[2 * rank + half, :, vcols]
            s = dot_t(q_ref[half, :, cols], k_blk)
            s = jnp.where(causal_mask(half_rows, half_rows), s, -jnp.inf)
            m = jnp.max(s, axis=1, keepdims=True)
            p = jnp.exp2((s - m) * log2e_scale)
            m_ref[half, h] = jnp.broadcast_to(m, (half_rows, dim))
            l_ref[half, h] = jnp.broadcast_to(jnp.sum(p, axis=1, keepdims=True), (half_rows, dim))
            acc_ref[half, h] = dot_n(p.astype(BF16), v_blk)

    def step(t, carry):
        late = (t >= rank).astype(jnp.int32)
        slot = block_slot(t - late * rank, n_sh)
        for h in range(heads):
            cols = slice(h * dim, (h + 1) * dim)
            vcols = slice(width + h * dim, width + (h + 1) * dim)
            k_blk = kv_buf[slot, :, cols]
            v_blk = kv_buf[slot, :, vcols]
            s = dot_t(q_ref[late, :, cols], k_blk)
            m_old = m_ref[late, h]
            m_new = jnp.maximum(m_old, jnp.max(s, axis=1, keepdims=True))
            factor = jnp.exp2((m_old - m_new) * log2e_scale)
            p = jnp.exp2((s - m_new[:, :1]) * log2e_scale)
            m_ref[late, h] = m_new
            l_ref[late, h] = l_ref[late, h] * factor + jnp.sum(p, axis=1, keepdims=True)
            acc_ref[late, h] = acc_ref[late, h] * factor + dot_n(p.astype(BF16), v_blk)
        return carry

    lax.fori_loop(0, 2 * n_sh - 1, step, 0)
    for half in range(2):
        for h in range(heads):
            cols = slice(h * dim, (h + 1) * dim)
            l = l_ref[half, h]
            o_ref[half, :, cols] = (acc_ref[half, h] / l).astype(BF16)
            lse = m_ref[half, h] * log2e_scale + jnp.log2(l)
            lse_ref[half, h:h + 1, :] = jnp.transpose(lse)[:1]


def stats_kernel(heads, dim, o_ref, do_ref, lse_ref, out_ref):
    half_rows = o_ref.shape[1]
    for half in range(2):
        rows = [lse_ref[half]]
        for h in range(heads):
            cols = slice(h * dim, (h + 1) * dim)
            prod = do_ref[half, :, cols].astype(F32) * o_ref[half, :, cols].astype(F32)
            delta = jnp.broadcast_to(jnp.sum(prod, axis=1, keepdims=True), (half_rows, dim))
            rows.append(jnp.transpose(delta)[:1])
        rows.append(jnp.zeros((8 - 2 * heads, half_rows), F32))
        out_ref[half] = jnp.concatenate(rows, axis=0)


def query_grad_kernel(n_sh, heads, dim, meta, rank_ref, q_ref, do_ref, st_ref, *rest):
    n_p = len(meta)
    kv_refs = rest[:n_p]
    dq_ref, kv_buf, acc_ref, lse_ref, dot_ref, sems = rest[n_p:]
    rank = rank_ref[0]
    width = heads * dim
    half_rows = q_ref.shape[1]
    scale = dim ** -0.5
    log2e_scale = math.log2(math.e) * scale
    copies = load_pieces(kv_refs, meta, kv_buf, sems, rank, n_sh)
    for half in range(2):
        for h in range(heads):
            lse_ref[half, h] = jnp.transpose(jnp.broadcast_to(st_ref[half, h:h + 1, :], (dim, half_rows)))
            dot_ref[half, h] = jnp.transpose(jnp.broadcast_to(st_ref[half, heads + h:heads + h + 1, :], (dim, half_rows)))
    for copy in copies:
        copy.wait()

    def contribution(half, slot, h, masked):
        cols = slice(h * dim, (h + 1) * dim)
        vcols = slice(width + h * dim, width + (h + 1) * dim)
        k_blk = kv_buf[slot, :, cols]
        v_blk = kv_buf[slot, :, vcols]
        s = dot_t(q_ref[half, :, cols], k_blk)
        p = jnp.exp2(s * log2e_scale - lse_ref[half, h][:, :1])
        if masked:
            p = jnp.where(causal_mask(half_rows, half_rows), p, 0.0)
        dp = dot_t(do_ref[half, :, cols], v_blk)
        ds = (p * (dp - dot_ref[half, h][:, :1])).astype(BF16)
        return dot_n(ds, k_blk)

    for half in range(2):
        for h in range(heads):
            acc_ref[half, h] = contribution(half, 2 * rank + half, h, True)

    def step(t, carry):
        late = (t >= rank).astype(jnp.int32)
        slot = block_slot(t - late * rank, n_sh)
        for h in range(heads):
            acc_ref[late, h] = acc_ref[late, h] + contribution(late, slot, h, False)
        return carry

    lax.fori_loop(0, 2 * n_sh - 1, step, 0)
    for half in range(2):
        for h in range(heads):
            dq_ref[half, :, h * dim:(h + 1) * dim] = (acc_ref[half, h] * scale).astype(BF16)


def key_grad_kernel(n_sh, heads, dim, meta, st_meta, rank_ref, kv_ref, *rest):
    n_p = len(meta)
    q_refs = rest[:n_p]
    do_refs = rest[n_p:2 * n_p]
    st_refs = rest[2 * n_p:2 * n_p + len(st_meta)]
    dkv_ref, q_buf, do_buf, st_buf, dk_acc, dv_acc, sems = rest[2 * n_p + len(st_meta):]
    rank = rank_ref[0]
    width = heads * dim
    half_rows = kv_ref.shape[1]
    scale = dim ** -0.5
    log2e_scale = math.log2(math.e) * scale
    copies = load_pieces(q_refs, meta, q_buf, sems.at[0], rank, n_sh)
    copies += load_pieces(do_refs, meta, do_buf, sems.at[1], rank, n_sh)
    for idx, (ref, shift) in enumerate(zip(st_refs, st_meta)):
        owner = lax.rem(rank + n_sh - shift, n_sh)
        copy = pltpu.make_async_copy(ref, st_buf.at[pl.ds(2 * owner, 2)], sems.at[2, idx])
        copy.start()
        copies.append(copy)
    for copy in copies:
        copy.wait()

    def contribution(half, slot, h, masked):
        cols = slice(h * dim, (h + 1) * dim)
        vcols = slice(width + h * dim, width + (h + 1) * dim)
        q_blk = q_buf[slot, :, cols]
        do_blk = do_buf[slot, :, cols]
        s = dot_t(kv_ref[half, :, cols], q_blk)
        p = jnp.exp2(s * log2e_scale - st_buf[slot, h:h + 1, :])
        if masked:
            p = jnp.where(causal_mask(half_rows, half_rows, transposed=True), p, 0.0)
        dp = dot_t(kv_ref[half, :, vcols], do_blk)
        ds = (p * (dp - st_buf[slot, heads + h:heads + h + 1, :])).astype(BF16)
        return dot_n(ds, q_blk), dot_n(p.astype(BF16), do_blk)

    for half in range(2):
        for h in range(heads):
            dk_acc[half, h], dv_acc[half, h] = contribution(half, 2 * rank + half, h, True)

    def step(t, carry):
        n_early = 2 * n_sh - 1 - rank
        late = (t >= n_early).astype(jnp.int32)
        slot = block_slot(jnp.where(late == 1, t + 1, rank + 1 + t), n_sh)
        for h in range(heads):
            dk_part, dv_part = contribution(late, slot, h, False)
            dk_acc[late, h] = dk_acc[late, h] + dk_part
            dv_acc[late, h] = dv_acc[late, h] + dv_part
        return carry

    lax.fori_loop(0, 2 * n_sh - 1, step, 0)
    for half in range(2):
        for h in range(heads):
            cols = slice(h * dim, (h + 1) * dim)
            vcols = slice(width + h * dim, width + (h + 1) * dim)
            dkv_ref[half, :, cols] = (dk_acc[half, h] * scale).astype(BF16)
            dkv_ref[half, :, vcols] = dv_acc[half, h].astype(BF16)


SMEM_SPEC = pl.BlockSpec(memory_space=pltpu.SMEM)
VMEM_SPEC = pl.BlockSpec(memory_space=pltpu.VMEM)
ANY_SPEC = pl.BlockSpec(memory_space=pl.ANY)


def attention_call(kernel, name, n_dots, work, in_specs, out_shape, scratch):
    many = isinstance(out_shape, (list, tuple))
    return pl.pallas_call(
        kernel,
        name=name,
        out_shape=out_shape,
        in_specs=in_specs,
        out_specs=[VMEM_SPEC] * len(out_shape) if many else VMEM_SPEC,
        scratch_shapes=scratch,
        cost_estimate=pl.CostEstimate(flops=4 * n_dots * work, bytes_accessed=10 * 2 ** 20, transcendentals=0),
        compiler_params=pltpu.CompilerParams(vmem_limit_bytes=VMEM_LIMIT),
    )


def solution(mesh):
    n_sh = mesh.shape["cp"]

    def device_fn(x_blk, w_query, w_key, w_value, w_out, dy_blk):
        rank = lax.axis_index("cp").astype(jnp.int32).reshape(1)
        model_dim, heads, dim = w_query.shape
        width = heads * dim
        wq = w_query.reshape(model_dim, width)
        wkv = jnp.concatenate([w_key.reshape(model_dim, width), w_value.reshape(model_dim, width)], axis=1)
        wo = w_out.reshape(width, model_dim)

        x_rows = lax.all_gather(x_blk, "tp", axis=0, tiled=True)
        dy_rows = lax.all_gather(dy_blk, "tp", axis=0, tiled=True)
        n_rows = x_rows.shape[0]
        half_rows = n_rows // 2
        pairs = (2 * n_sh + 1) * half_rows * half_rows * heads * dim

        kv = dot_n(x_rows, wkv).astype(BF16).reshape(2, half_rows, 2 * width)
        kv_pieces = shard_pieces(kv, n_sh)
        q = dot_n(x_rows, wq).astype(BF16).reshape(2, half_rows, width)
        q_pieces = shard_pieces(q, n_sh)
        d_o = dot_t(dy_rows, wo).astype(BF16).reshape(2, half_rows, width)
        do_pieces = shard_pieces(d_o, n_sh)
        meta = [piece[1:] for piece in kv_pieces]
        n_p = len(meta)
        acc = pltpu.VMEM((2, heads, half_rows, dim), F32)

        o, lse = attention_call(
            functools.partial(forward_kernel, n_sh, heads, dim, meta), "attn_fwd", 2, pairs // 2,
            [SMEM_SPEC, VMEM_SPEC] + [ANY_SPEC] * n_p,
            [jax.ShapeDtypeStruct((2, half_rows, width), BF16), jax.ShapeDtypeStruct((2, heads, half_rows), F32)],
            [pltpu.VMEM((2 * n_sh, half_rows, 2 * width), BF16), acc, acc, acc, pltpu.SemaphoreType.DMA((n_p,))],
        )(rank, q, *[piece[0] for piece in kv_pieces])
        o_flat = o.reshape(n_rows, width)
        y_part = dot_n(o_flat, wo)
        y_blk = lax.psum_scatter(y_part, "tp", scatter_dimension=0, tiled=True).astype(BF16)

        stats = pl.pallas_call(
            functools.partial(stats_kernel, heads, dim),
            name="attn_stats",
            out_shape=jax.ShapeDtypeStruct((2, 8, half_rows), F32),
        )(o, d_o, lse)
        st_meta = list(range(n_sh))
        st_pieces = [stats] + [
            lax.ppermute(stats, "cp", [(src, (src + shift) % n_sh) for src in range(n_sh)]) for shift in st_meta[1:]]

        dq = attention_call(
            functools.partial(query_grad_kernel, n_sh, heads, dim, meta), "attn_dq", 3, pairs // 2,
            [SMEM_SPEC, VMEM_SPEC, VMEM_SPEC, VMEM_SPEC] + [ANY_SPEC] * n_p,
            jax.ShapeDtypeStruct((2, half_rows, width), BF16),
            [pltpu.VMEM((2 * n_sh, half_rows, 2 * width), BF16), acc, acc, acc, pltpu.SemaphoreType.DMA((n_p,))],
        )(rank, q, d_o, stats, *[piece[0] for piece in kv_pieces])
        dkv = attention_call(
            functools.partial(key_grad_kernel, n_sh, heads, dim, meta, st_meta), "attn_dkv", 4, pairs // 2,
            [SMEM_SPEC, VMEM_SPEC] + [ANY_SPEC] * (2 * n_p + n_sh),
            jax.ShapeDtypeStruct((2, half_rows, 2 * width), BF16),
            [pltpu.VMEM((2 * n_sh, half_rows, width), BF16), pltpu.VMEM((2 * n_sh, half_rows, width), BF16),
             pltpu.VMEM((2 * n_sh, 8, half_rows), F32), acc, acc, pltpu.SemaphoreType.DMA((3, max(n_p, n_sh)))],
        )(rank, kv, *[piece[0] for piece in q_pieces], *[piece[0] for piece in do_pieces], *st_pieces)

        dq_flat = dq.reshape(n_rows, width)
        dkv_flat = dkv.reshape(n_rows, 2 * width)
        d_all = jnp.concatenate([dq_flat, dkv_flat], axis=1)
        w_all = jnp.concatenate([wq, wkv], axis=1)
        dx_part = dot_t(d_all, w_all)
        dx_blk = lax.psum_scatter(dx_part, "tp", scatter_dimension=0, tiled=True).astype(BF16)

        def weight_grad(lhs, rhs, shape):
            return lax.dot_general(lhs, rhs, ROWS_CONTRACT, preferred_element_type=F32).astype(BF16).reshape(shape)[None]

        grad_wo = weight_grad(o_flat, dy_rows, (heads, dim, model_dim))
        grad_wq = weight_grad(x_rows, dq_flat, (model_dim, heads, dim))
        grad_wk = weight_grad(x_rows, dkv_flat[:, :width], (model_dim, heads, dim))
        grad_wv = weight_grad(x_rows, dkv_flat[:, width:], (model_dim, heads, dim))
        return y_blk, dx_blk, grad_wq, grad_wk, grad_wv, grad_wo

    return jax.shard_map(device_fn, mesh=mesh,
                         in_specs=(ROW_SPEC, HEAD_SPEC, HEAD_SPEC, HEAD_SPEC, OUT_W_SPEC, ROW_SPEC),
                         out_specs=(ROW_SPEC, ROW_SPEC, GRAD_SPEC, GRAD_SPEC, GRAD_SPEC, GRAD_OUT_SPEC),
                         check_vma=False)
```

```python
import functools
import math

import jax
import jax.numpy as jnp
from jax import lax
from jax.experimental import pallas as pl
from jax.experimental.pallas import tpu as pltpu
from jax.sharding import PartitionSpec as P

ROW_SPEC = P(("dp", "cp", "tp"), None)
HEAD_SPEC = P(None, "tp", None)
OUT_W_SPEC = P("tp", None, None)
GRAD_SPEC = P(("dp", "cp"), None, "tp", None)
GRAD_OUT_SPEC = P(("dp", "cp"), "tp", None, None)
COLS_CONTRACT = (((1,), (1,)), ((), ()))
ROWS_CONTRACT = (((0,), (0,)), ((), ()))
VMEM_LIMIT = 58 * 1024 * 1024
F32 = jnp.float32
BF16 = jnp.bfloat16


def dot_t(lhs, rhs):
    return lax.dot_general(lhs, rhs, COLS_CONTRACT, preferred_element_type=F32)


def dot_n(lhs, rhs):
    return jnp.dot(lhs, rhs, preferred_element_type=F32)


def block_slot(pos_blk, n_sh):
    return jnp.where(pos_blk < n_sh, 2 * pos_blk, 2 * (2 * n_sh - 1 - pos_blk) + 1)


def shard_exchange(n_sh, pairs, sends, recvs):
    n_x = n_sh // 2
    rank = lax.axis_index("cp")
    chip, core = rank // 2, lax.rem(rank, 2)

    def rank_of(dx, dc):
        return 2 * lax.rem(chip + dx, n_x) + lax.rem(core + dc, 2)

    n_kinds = 9
    kinds = {"prev": 0, "next": 1, "far_lo": 2, "far_hi": 3, "own_x": 4, "prev_x": 5, "next_x": 6, "far_lo_x": 7, "far_hi_x": 8}

    def part(buf, dx, dc, half):
        return buf.at[pl.ds(2 * rank_of(dx, dc) + (0 if half is None else half), 2 if half is None else 1)]

    routes = {
        "prev": ((0, 0), None, (1, 0)), "next": ((0, 0), None, (n_x - 1, 0)), "own_x": ((0, 0), None, (0, 1)),
        "far_lo": ((n_x - 1, 0), 0, (1, 0)), "far_hi": ((1, 0), 1, (n_x - 1, 0)),
        "prev_x": ((n_x - 1, 0), None, (0, 1)), "next_x": ((1, 0), None, (0, 1)),
        "far_lo_x": ((2, 0), 0, (0, 1)), "far_hi_x": ((2, 0), 1, (0, 1)),
    }

    def copies(kind):
        (dx, dc), half, target = routes[kind]
        out = []
        for idx, (own, buf) in enumerate(pairs):
            dst = part(buf, dx, dc, half)
            src = own if (dx, dc) == (0, 0) else dst
            out.append(pltpu.make_async_remote_copy(
                src_ref=src, dst_ref=dst, send_sem=sends.at[idx * n_kinds + kinds[kind]], recv_sem=recvs.at[idx * n_kinds + kinds[kind]],
                device_id={"cp": rank_of(*target)}, device_id_type=pl.DeviceIdType.MESH))
        return out

    def start(*names):
        for name in names:
            for copy in copies(name):
                copy.start()

    def wait_recv(*names):
        for name in names:
            for copy in copies(name):
                copy.wait_recv()

    def wait_sends():
        for name in routes:
            for copy in copies(name):
                copy.wait_send()

    def barrier():
        sem = pltpu.get_barrier_semaphore()
        for target in ((1, 0), (n_x - 1, 0), (0, 1)):
            pl.semaphore_signal(sem, inc=1, device_id={"cp": rank_of(*target)}, device_id_type=pl.DeviceIdType.MESH)
        pl.semaphore_wait(sem, 3)

    return rank, rank_of, barrier, start, wait_recv, wait_sends


def causal_mask(rows, cols, transposed=False):
    row_ids = lax.broadcasted_iota(jnp.int32, (rows, cols), 0)
    col_ids = lax.broadcasted_iota(jnp.int32, (rows, cols), 1)
    return col_ids >= row_ids if transposed else row_ids >= col_ids


def forward_kernel(n_sh, heads, dim, q_ref, kv_ref, o_ref, lse_ref, all_ref, kv_buf, m_ref, l_ref, acc_ref, sends, recvs, sems):
    rank, rank_of, barrier, start, wait_recv, wait_sends = shard_exchange(n_sh, [(kv_ref, kv_buf)], sends, recvs)
    n_x = n_sh // 2
    barrier()
    start("prev", "next", "own_x")
    width = heads * dim
    half_rows = q_ref.shape[1]
    log2e_scale = math.log2(math.e) * dim ** -0.5
    own = pltpu.make_async_copy(kv_ref, kv_buf.at[pl.ds(2 * rank, 2)], sems.at[0])
    own.start()
    own.wait()
    for half in range(2):
        for h in range(heads):
            cols = slice(h * dim, (h + 1) * dim)
            vcols = slice(width + h * dim, width + (h + 1) * dim)
            k_blk = kv_buf[2 * rank + half, :, cols]
            v_blk = kv_buf[2 * rank + half, :, vcols]
            s = dot_t(q_ref[half, :, cols], k_blk)
            s = jnp.where(causal_mask(half_rows, half_rows), s, -jnp.inf)
            m = jnp.max(s, axis=1, keepdims=True)
            p = jnp.exp2((s - m) * log2e_scale)
            m_ref[half, h] = jnp.broadcast_to(m, (half_rows, dim))
            l_ref[half, h] = jnp.broadcast_to(jnp.sum(p, axis=1, keepdims=True), (half_rows, dim))
            acc_ref[half, h] = dot_n(p.astype(BF16), v_blk)

    def unit(late, slot):
        for h in range(heads):
            cols = slice(h * dim, (h + 1) * dim)
            vcols = slice(width + h * dim, width + (h + 1) * dim)
            k_blk = kv_buf[slot, :, cols]
            v_blk = kv_buf[slot, :, vcols]
            s = dot_t(q_ref[late, :, cols], k_blk)
            m_old = m_ref[late, h]
            m_new = jnp.maximum(m_old, jnp.max(s, axis=1, keepdims=True))
            factor = jnp.exp2((m_old - m_new) * log2e_scale)
            p = jnp.exp2((s - m_new[:, :1]) * log2e_scale)
            m_ref[late, h] = m_new
            l_ref[late, h] = l_ref[late, h] * factor + jnp.sum(p, axis=1, keepdims=True)
            acc_ref[late, h] = acc_ref[late, h] * factor + dot_n(p.astype(BF16), v_blk)

    def visit(first, count, shard_of):
        def step(t, carry):
            shard = shard_of(t // 2)
            after = (shard > rank).astype(jnp.int32)
            second = lax.rem(t, 2)
            late = jnp.where(second == 1, after, 1)
            slot = 2 * shard + jnp.where(second == 1, after, 0)
            unit(late, slot)
            return carry
        lax.fori_loop(first, first + count, step, 0)

    offsets = [(0, 0), (0, 1), (n_x - 1, 0), (1, 0), (n_x - 1, 1), (1, 1), (2, 0), (2, 1)]

    def shard_of(idx):
        out = rank_of(*offsets[0])
        for pos in range(1, n_sh):
            out = jnp.where(idx == pos, rank_of(*offsets[pos]), out)
        return out

    visit(0, 1, shard_of)
    wait_recv("own_x")
    visit(2, 2, shard_of)
    wait_recv("prev")
    start("far_lo", "prev_x")
    wait_recv("next")
    start("far_hi", "next_x")
    visit(4, 4, shard_of)
    wait_recv("prev_x", "next_x")
    visit(8, 2, shard_of)
    wait_recv("far_lo", "far_hi")
    start("far_lo_x", "far_hi_x")
    visit(10, 4, shard_of)
    wait_recv("far_lo_x", "far_hi_x")
    out = pltpu.make_async_copy(kv_buf, all_ref, sems.at[0])
    out.start()
    visit(14, 2, shard_of)
    for half in range(2):
        for h in range(heads):
            cols = slice(h * dim, (h + 1) * dim)
            l = l_ref[half, h]
            o_ref[half, :, cols] = (acc_ref[half, h] / l).astype(BF16)
            lse = m_ref[half, h] * log2e_scale + jnp.log2(l)
            lse_ref[half, h:h + 1, :] = jnp.transpose(lse)[:1]
    out.wait()
    wait_sends()


def stats_kernel(heads, dim, o_ref, do_ref, lse_ref, out_ref):
    half_rows = o_ref.shape[1]
    for half in range(2):
        rows = [lse_ref[half]]
        for h in range(heads):
            cols = slice(h * dim, (h + 1) * dim)
            prod = do_ref[half, :, cols].astype(F32) * o_ref[half, :, cols].astype(F32)
            delta = jnp.broadcast_to(jnp.sum(prod, axis=1, keepdims=True), (half_rows, dim))
            rows.append(jnp.transpose(delta)[:1])
        rows.append(jnp.zeros((8 - 2 * heads, half_rows), F32))
        out_ref[half] = jnp.concatenate(rows, axis=0)


def backward_kernel(n_sh, heads, dim, q_ref, do_ref, st_ref, all_ref, dq_ref, dkv_ref,
                    kv_buf, q_buf, do_buf, st_buf, acc_ref, lse_ref, dot_ref, dk_acc, dv_acc, sends, recvs, sems):
    rank, rank_of, barrier, start, wait_recv, wait_sends = shard_exchange(
        n_sh, [(q_ref, q_buf), (do_ref, do_buf), (st_ref, st_buf)], sends, recvs)
    n_x = n_sh // 2
    barrier()
    start("prev", "next", "own_x")
    load = [pltpu.make_async_copy(all_ref, kv_buf, sems.at[0])]
    for idx, (own, buf) in enumerate([(q_ref, q_buf), (do_ref, do_buf), (st_ref, st_buf)]):
        load.append(pltpu.make_async_copy(own, buf.at[pl.ds(2 * rank, 2)], sems.at[1 + idx]))
    for copy in load:
        copy.start()
    width = heads * dim
    half_rows = q_ref.shape[1]
    scale = dim ** -0.5
    log2e_scale = math.log2(math.e) * scale
    for half in range(2):
        for h in range(heads):
            lse_ref[half, h] = jnp.transpose(jnp.broadcast_to(st_ref[half, h:h + 1, :], (dim, half_rows)))
            dot_ref[half, h] = jnp.transpose(jnp.broadcast_to(st_ref[half, heads + h:heads + h + 1, :], (dim, half_rows)))
    for copy in load:
        copy.wait()

    def query_part(half, slot, h, masked):
        cols = slice(h * dim, (h + 1) * dim)
        vcols = slice(width + h * dim, width + (h + 1) * dim)
        k_blk = kv_buf[slot, :, cols]
        v_blk = kv_buf[slot, :, vcols]
        s = dot_t(q_ref[half, :, cols], k_blk)
        p = jnp.exp2(s * log2e_scale - lse_ref[half, h][:, :1])
        if masked:
            p = jnp.where(causal_mask(half_rows, half_rows), p, 0.0)
        dp = dot_t(do_ref[half, :, cols], v_blk)
        ds = (p * (dp - dot_ref[half, h][:, :1])).astype(BF16)
        return dot_n(ds, k_blk)

    for half in range(2):
        for h in range(heads):
            acc_ref[half, h] = query_part(half, 2 * rank + half, h, True)

    def query_step(t, carry):
        late = (t >= rank).astype(jnp.int32)
        slot = block_slot(t - late * rank, n_sh)
        for h in range(heads):
            acc_ref[late, h] = acc_ref[late, h] + query_part(late, slot, h, False)
        return carry

    lax.fori_loop(0, 2 * n_sh - 1, query_step, 0)
    wait_recv("prev")
    start("far_lo", "prev_x")
    wait_recv("next")
    start("far_hi", "next_x")
    for half in range(2):
        for h in range(heads):
            dq_ref[half, :, h * dim:(h + 1) * dim] = (acc_ref[half, h] * scale).astype(BF16)

    def key_part(half, slot, h, masked):
        cols = slice(h * dim, (h + 1) * dim)
        vcols = slice(width + h * dim, width + (h + 1) * dim)
        q_blk = q_buf[slot, :, cols]
        do_blk = do_buf[slot, :, cols]
        k_slot = 2 * rank + half
        s = dot_t(kv_buf[k_slot, :, cols], q_blk)
        p = jnp.exp2(s * log2e_scale - st_buf[slot, h:h + 1, :])
        if masked:
            p = jnp.where(causal_mask(half_rows, half_rows, transposed=True), p, 0.0)
        dp = dot_t(kv_buf[k_slot, :, vcols], do_blk)
        ds = (p * (dp - st_buf[slot, heads + h:heads + h + 1, :])).astype(BF16)
        return dot_n(ds, q_blk), dot_n(p.astype(BF16), do_blk)

    for half in range(2):
        for h in range(heads):
            dk_acc[half, h], dv_acc[half, h] = key_part(half, 2 * rank + half, h, True)

    offsets = [(0, 0), (0, 1), (n_x - 1, 0), (1, 0), (n_x - 1, 1), (1, 1), (2, 0), (2, 1)]

    def visit(first, count):
        def step(t, carry):
            idx = t // 2
            shard = rank_of(*offsets[0])
            for pos in range(1, n_sh):
                shard = jnp.where(idx == pos, rank_of(*offsets[pos]), shard)
            before = (shard < rank).astype(jnp.int32)
            second = lax.rem(t, 2)
            late = jnp.where(second == 1, before, 0)
            slot = 2 * shard + jnp.where(second == 1, before, 1)
            for h in range(heads):
                dk_part, dv_part = key_part(late, slot, h, False)
                dk_acc[late, h] = dk_acc[late, h] + dk_part
                dv_acc[late, h] = dv_acc[late, h] + dv_part
            return carry
        lax.fori_loop(first, first + count, step, 0)

    visit(0, 1)
    wait_recv("own_x")
    visit(2, 6)
    wait_recv("prev_x", "next_x")
    visit(8, 2)
    wait_recv("far_lo", "far_hi")
    start("far_lo_x", "far_hi_x")
    visit(10, 4)
    wait_recv("far_lo_x", "far_hi_x")
    visit(14, 2)
    for half in range(2):
        for h in range(heads):
            cols = slice(h * dim, (h + 1) * dim)
            vcols = slice(width + h * dim, width + (h + 1) * dim)
            dkv_ref[half, :, cols] = (dk_acc[half, h] * scale).astype(BF16)
            dkv_ref[half, :, vcols] = dv_acc[half, h].astype(BF16)
    wait_sends()


VMEM_SPEC = pl.BlockSpec(memory_space=pltpu.VMEM)
ANY_SPEC = pl.BlockSpec(memory_space=pl.ANY)


def attention_call(kernel, name, collective_id, flops, in_specs, out_specs, out_shape, scratch):
    return pl.pallas_call(
        kernel,
        name=name,
        out_shape=out_shape,
        in_specs=in_specs,
        out_specs=out_specs,
        scratch_shapes=scratch,
        cost_estimate=pl.CostEstimate(flops=flops, bytes_accessed=10 * 2 ** 20, transcendentals=0),
        compiler_params=pltpu.CompilerParams(vmem_limit_bytes=VMEM_LIMIT, collective_id=collective_id, has_side_effects=True),
    )


def solution(mesh):
    n_sh = mesh.shape["cp"]

    def device_fn(x_blk, w_query, w_key, w_value, w_out, dy_blk):
        model_dim, heads, dim = w_query.shape
        width = heads * dim
        wq = w_query.reshape(model_dim, width)
        wkv = jnp.concatenate([w_key.reshape(model_dim, width), w_value.reshape(model_dim, width)], axis=1)
        wo = w_out.reshape(width, model_dim)

        x_rows = lax.all_gather(x_blk, "tp", axis=0, tiled=True)
        dy_rows = lax.all_gather(dy_blk, "tp", axis=0, tiled=True)
        n_rows = x_rows.shape[0]
        half_rows = n_rows // 2
        tile_flops = 4 * (2 * n_sh + 1) * half_rows * half_rows * heads * dim

        kv = dot_n(x_rows, wkv).astype(BF16).reshape(2, half_rows, 2 * width)
        q = dot_n(x_rows, wq).astype(BF16).reshape(2, half_rows, width)
        acc = pltpu.VMEM((2, heads, half_rows, dim), F32)
        dma = pltpu.SemaphoreType.DMA
        kv_all_shape = (2 * n_sh, half_rows, 2 * width)

        o, lse, kv_all = attention_call(
            functools.partial(forward_kernel, n_sh, heads, dim), "attn_fwd", 0, 2 * tile_flops,
            [VMEM_SPEC, VMEM_SPEC], [VMEM_SPEC, VMEM_SPEC, ANY_SPEC],
            [jax.ShapeDtypeStruct((2, half_rows, width), BF16), jax.ShapeDtypeStruct((2, heads, half_rows), F32),
             jax.ShapeDtypeStruct(kv_all_shape, BF16)],
            [pltpu.VMEM(kv_all_shape, BF16), acc, acc, acc, dma((9,)), dma((9,)), dma((1,))],
        )(q, kv)
        o_flat = o.reshape(n_rows, width)
        y_part = dot_n(o_flat, wo)
        y_blk = lax.psum_scatter(y_part, "tp", scatter_dimension=0, tiled=True).astype(BF16)

        d_o = dot_t(dy_rows, wo).astype(BF16).reshape(2, half_rows, width)
        stats = pl.pallas_call(
            functools.partial(stats_kernel, heads, dim),
            name="attn_stats",
            out_shape=jax.ShapeDtypeStruct((2, 8, half_rows), F32),
        )(o, d_o, lse)
        shard_buf = pltpu.VMEM((2 * n_sh, half_rows, width), BF16)
        dq, dkv = attention_call(
            functools.partial(backward_kernel, n_sh, heads, dim), "attn_bwd", 1, 7 * tile_flops // 2,
            [VMEM_SPEC, VMEM_SPEC, VMEM_SPEC, ANY_SPEC], [VMEM_SPEC, VMEM_SPEC],
            [jax.ShapeDtypeStruct((2, half_rows, width), BF16), jax.ShapeDtypeStruct((2, half_rows, 2 * width), BF16)],
            [pltpu.VMEM(kv_all_shape, BF16), shard_buf, shard_buf, pltpu.VMEM((2 * n_sh, 8, half_rows), F32),
             acc, acc, acc, acc, acc, dma((27,)), dma((27,)), dma((4,))],
        )(q, d_o, stats, kv_all)

        dq_flat = dq.reshape(n_rows, width)
        dkv_flat = dkv.reshape(n_rows, 2 * width)
        d_all = jnp.concatenate([dq_flat, dkv_flat], axis=1)
        w_all = jnp.concatenate([wq, wkv], axis=1)
        dx_part = dot_t(d_all, w_all)
        dx_blk = lax.psum_scatter(dx_part, "tp", scatter_dimension=0, tiled=True).astype(BF16)

        def weight_grad(lhs, rhs, shape):
            return lax.dot_general(lhs, rhs, ROWS_CONTRACT, preferred_element_type=F32).astype(BF16).reshape(shape)[None]

        grad_wo = weight_grad(o_flat, dy_rows, (heads, dim, model_dim))
        grad_wq = weight_grad(x_rows, dq_flat, (model_dim, heads, dim))
        grad_wk = weight_grad(x_rows, dkv_flat[:, :width], (model_dim, heads, dim))
        grad_wv = weight_grad(x_rows, dkv_flat[:, width:], (model_dim, heads, dim))
        return y_blk, dx_blk, grad_wq, grad_wk, grad_wv, grad_wo

    return jax.shard_map(device_fn, mesh=mesh,
                         in_specs=(ROW_SPEC, HEAD_SPEC, HEAD_SPEC, HEAD_SPEC, OUT_W_SPEC, ROW_SPEC),
                         out_specs=(ROW_SPEC, ROW_SPEC, GRAD_SPEC, GRAD_SPEC, GRAD_SPEC, GRAD_OUT_SPEC),
                         check_vma=False)
```

```python
import functools
import math

import jax
import jax.numpy as jnp
from jax import lax
from jax.experimental import pallas as pl
from jax.experimental.pallas import tpu as pltpu
from jax.sharding import PartitionSpec as P

ROW_SPEC = P(("dp", "cp", "tp"), None)
HEAD_SPEC = P(None, "tp", None)
OUT_W_SPEC = P("tp", None, None)
GRAD_SPEC = P(("dp", "cp"), None, "tp", None)
GRAD_OUT_SPEC = P(("dp", "cp"), "tp", None, None)
COLS_CONTRACT = (((1,), (1,)), ((), ()))
ROWS_CONTRACT = (((0,), (0,)), ((), ()))
VMEM_LIMIT = 58 * 1024 * 1024
F32 = jnp.float32
BF16 = jnp.bfloat16


def dot_t(lhs, rhs):
    return lax.dot_general(lhs, rhs, COLS_CONTRACT, preferred_element_type=F32)


def dot_n(lhs, rhs):
    return jnp.dot(lhs, rhs, preferred_element_type=F32)


LINE = 4


def block_slot(pos_blk, n_sh):
    return jnp.where(pos_blk < n_sh, 2 * pos_blk, 2 * (2 * n_sh - 1 - pos_blk) + 1)


def shard_exchange(n_sh, pairs, sends, recvs):
    n_x = n_sh // 2
    rank = lax.axis_index("cp")
    chip, core = rank // 2, lax.rem(rank, 2)

    def rank_of(dx, dc):
        return 2 * lax.rem(chip + dx, n_x) + lax.rem(core + dc, 2)

    n_kinds = 9
    kinds = {"prev": 0, "next": 1, "far_lo": 2, "far_hi": 3, "own_x": 4, "prev_x": 5, "next_x": 6, "far_lo_x": 7, "far_hi_x": 8}

    def part(buf, dx, dc, half):
        return buf.at[pl.ds(2 * rank_of(dx, dc) + (0 if half is None else half), 2 if half is None else 1)]

    routes = {
        "prev": ((0, 0), None, (1, 0)), "next": ((0, 0), None, (n_x - 1, 0)), "own_x": ((0, 0), None, (0, 1)),
        "far_lo": ((n_x - 1, 0), 0, (1, 0)), "far_hi": ((1, 0), 1, (n_x - 1, 0)),
        "prev_x": ((n_x - 1, 0), None, (0, 1)), "next_x": ((1, 0), None, (0, 1)),
        "far_lo_x": ((2, 0), 0, (0, 1)), "far_hi_x": ((2, 0), 1, (0, 1)),
    }

    def copies(kind):
        (dx, dc), half, target = routes[kind]
        out = []
        for idx, (own, buf) in enumerate(pairs):
            dst = part(buf, dx, dc, half)
            src = own if (dx, dc) == (0, 0) else dst
            out.append(pltpu.make_async_remote_copy(
                src_ref=src, dst_ref=dst, send_sem=sends.at[idx * n_kinds + kinds[kind]], recv_sem=recvs.at[idx * n_kinds + kinds[kind]],
                device_id={"cp": rank_of(*target)}, device_id_type=pl.DeviceIdType.MESH))
        return out

    def start(*names):
        for name in names:
            for copy in copies(name):
                copy.start()

    def wait_recv(*names):
        for name in names:
            for copy in copies(name):
                copy.wait_recv()

    def wait_sends():
        for name in routes:
            for copy in copies(name):
                copy.wait_send()

    def barrier(others=()):
        sem = pltpu.get_barrier_semaphore()
        for target in [{"cp": rank_of(*offset)} for offset in ((1, 0), (n_x - 1, 0), (0, 1))] + list(others):
            pl.semaphore_signal(sem, inc=1, device_id=target, device_id_type=pl.DeviceIdType.MESH)
        pl.semaphore_wait(sem, 3 + len(others))

    return rank, rank_of, barrier, start, wait_recv, wait_sends


def line_device(shift):
    tp_idx = lax.axis_index("tp")
    return {"tp": LINE * (tp_idx // LINE) + lax.rem(lax.rem(tp_idx, LINE) + shift + LINE, LINE)}


def weight_gather(w_ref, all_ref, other_core, sends, recvs):
    core = lax.rem(lax.axis_index("cp"), 2)
    part_rows = w_ref.shape[0] // 2
    quarter = part_rows // 2
    first = core * part_rows

    def whole(slot):
        return all_ref.at[slot, pl.ds(first, part_rows)]

    def lo(slot):
        return all_ref.at[slot, pl.ds(first, quarter)]

    def hi(slot):
        return all_ref.at[slot, pl.ds(first + quarter, quarter)]

    own = w_ref.at[pl.ds(first, part_rows)]
    routes = [
        ("prev", own, whole(1), line_device(1)), ("next", own, whole(2), line_device(-1)),
        ("far_lo", lo(1), lo(3), line_device(1)), ("far_hi", hi(2), hi(3), line_device(-1)),
        ("prev_x", whole(1), whole(1), other_core), ("next_x", whole(2), whole(2), other_core),
        ("far_lo_x", lo(3), lo(3), other_core), ("far_hi_x", hi(3), hi(3), other_core),
    ]

    def copy_of(name):
        for idx, (kind, src, dst, target) in enumerate(routes):
            if kind == name:
                return pltpu.make_async_remote_copy(src_ref=src, dst_ref=dst, send_sem=sends.at[idx], recv_sem=recvs.at[idx],
                                                    device_id=target, device_id_type=pl.DeviceIdType.MESH)

    def start(*names):
        for name in names:
            copy_of(name).start()

    def wait_recv(*names):
        for name in names:
            copy_of(name).wait_recv()

    def wait_sends():
        for route in routes:
            copy_of(route[0]).wait_send()

    return start, wait_recv, wait_sends


def causal_mask(rows, cols, transposed=False):
    row_ids = lax.broadcasted_iota(jnp.int32, (rows, cols), 0)
    col_ids = lax.broadcasted_iota(jnp.int32, (rows, cols), 1)
    return col_ids >= row_ids if transposed else row_ids >= col_ids


def forward_kernel(n_sh, heads, dim, q_ref, kv_ref, wo_ref, o_ref, lse_ref, all_ref, wo_all_ref,
                   kv_buf, m_ref, l_ref, acc_ref, sends, recvs, w_sends, w_recvs, sems):
    rank, rank_of, barrier, start, wait_recv, wait_sends = shard_exchange(n_sh, [(kv_ref, kv_buf)], sends, recvs)
    n_x = n_sh // 2
    w_start, w_wait, w_wait_sends = weight_gather(wo_ref, wo_all_ref, {"cp": rank_of(0, 1)}, w_sends, w_recvs)
    barrier([line_device(1), line_device(-1)])
    start("prev", "next", "own_x")
    w_start("prev", "next")
    width = heads * dim
    half_rows = q_ref.shape[1]
    log2e_scale = math.log2(math.e) * dim ** -0.5
    own_w = pltpu.make_async_copy(wo_ref, wo_all_ref.at[0], sems.at[1])
    own_w.start()
    own = pltpu.make_async_copy(kv_ref, kv_buf.at[pl.ds(2 * rank, 2)], sems.at[0])
    own.start()
    own.wait()
    for half in range(2):
        for h in range(heads):
            cols = slice(h * dim, (h + 1) * dim)
            vcols = slice(width + h * dim, width + (h + 1) * dim)
            k_blk = kv_buf[2 * rank + half, :, cols]
            v_blk = kv_buf[2 * rank + half, :, vcols]
            s = dot_t(q_ref[half, :, cols], k_blk)
            s = jnp.where(causal_mask(half_rows, half_rows), s, -jnp.inf)
            m = jnp.max(s, axis=1, keepdims=True)
            p = jnp.exp2((s - m) * log2e_scale)
            m_ref[half, h] = jnp.broadcast_to(m, (half_rows, dim))
            l_ref[half, h] = jnp.broadcast_to(jnp.sum(p, axis=1, keepdims=True), (half_rows, dim))
            acc_ref[half, h] = dot_n(p.astype(BF16), v_blk)

    def unit(late, slot):
        for h in range(heads):
            cols = slice(h * dim, (h + 1) * dim)
            vcols = slice(width + h * dim, width + (h + 1) * dim)
            k_blk = kv_buf[slot, :, cols]
            v_blk = kv_buf[slot, :, vcols]
            s = dot_t(q_ref[late, :, cols], k_blk)
            m_old = m_ref[late, h]
            m_new = jnp.maximum(m_old, jnp.max(s, axis=1, keepdims=True))
            factor = jnp.exp2((m_old - m_new) * log2e_scale)
            p = jnp.exp2((s - m_new[:, :1]) * log2e_scale)
            m_ref[late, h] = m_new
            l_ref[late, h] = l_ref[late, h] * factor + jnp.sum(p, axis=1, keepdims=True)
            acc_ref[late, h] = acc_ref[late, h] * factor + dot_n(p.astype(BF16), v_blk)

    def visit(first, count, shard_of):
        def step(t, carry):
            shard = shard_of(t // 2)
            after = (shard > rank).astype(jnp.int32)
            second = lax.rem(t, 2)
            late = jnp.where(second == 1, after, 1)
            slot = 2 * shard + jnp.where(second == 1, after, 0)
            unit(late, slot)
            return carry
        lax.fori_loop(first, first + count, step, 0)

    offsets = [(0, 0), (0, 1), (n_x - 1, 0), (1, 0), (n_x - 1, 1), (1, 1), (2, 0), (2, 1)]

    def shard_of(idx):
        out = rank_of(*offsets[0])
        for pos in range(1, n_sh):
            out = jnp.where(idx == pos, rank_of(*offsets[pos]), out)
        return out

    visit(0, 1, shard_of)
    wait_recv("own_x")
    visit(2, 2, shard_of)
    wait_recv("prev")
    start("far_lo", "prev_x")
    wait_recv("next")
    start("far_hi", "next_x")
    visit(4, 4, shard_of)
    w_wait("prev")
    w_start("far_lo", "prev_x")
    w_wait("next")
    w_start("far_hi", "next_x")
    wait_recv("prev_x", "next_x")
    visit(8, 2, shard_of)
    wait_recv("far_lo", "far_hi")
    start("far_lo_x", "far_hi_x")
    visit(10, 4, shard_of)
    wait_recv("far_lo_x", "far_hi_x")
    out = pltpu.make_async_copy(kv_buf, all_ref, sems.at[0])
    out.start()
    visit(14, 2, shard_of)
    w_wait("far_lo", "far_hi")
    w_start("far_lo_x", "far_hi_x")
    for half in range(2):
        for h in range(heads):
            cols = slice(h * dim, (h + 1) * dim)
            l = l_ref[half, h]
            o_ref[half, :, cols] = (acc_ref[half, h] / l).astype(BF16)
            lse = m_ref[half, h] * log2e_scale + jnp.log2(l)
            lse_ref[half, h:h + 1, :] = jnp.transpose(lse)[:1]
    out.wait()
    own_w.wait()
    w_wait("prev_x", "next_x", "far_lo_x", "far_hi_x")
    wait_sends()
    w_wait_sends()


def stats_kernel(heads, dim, o_ref, do_ref, lse_ref, out_ref, rows_ref, o_buf, sends, recvs):
    y_pos = lax.rem(lax.axis_index("tp"), LINE)
    shifts = (0, 1, -1, 2)
    sem = pltpu.get_barrier_semaphore()
    for shift in shifts[1:]:
        pl.semaphore_signal(sem, inc=1, device_id=line_device(shift), device_id_type=pl.DeviceIdType.MESH)
    pl.semaphore_wait(sem, 3)
    copies = []
    for slot in range(1, LINE):
        target = line_device(shifts[slot])
        copies.append(pltpu.make_async_remote_copy(
            src_ref=o_ref.at[:, lax.rem(target["tp"], LINE)], dst_ref=o_buf.at[slot - 1], send_sem=sends.at[slot - 1],
            recv_sem=recvs.at[slot - 1], device_id=target, device_id_type=pl.DeviceIdType.MESH))
        copies[-1].start()
    width = heads * dim
    rows_ref[:, :, :width] = o_ref[:, y_pos]
    half_rows = lse_ref.shape[2]
    o_rows = o_ref[...].reshape(2, half_rows, width)
    for half in range(2):
        rows = [lse_ref[half]]
        for h in range(heads):
            cols = slice(h * dim, (h + 1) * dim)
            prod = do_ref[half, :, cols].astype(F32) * o_rows[half, :, cols].astype(F32)
            delta = jnp.broadcast_to(jnp.sum(prod, axis=1, keepdims=True), (half_rows, dim))
            rows.append(jnp.transpose(delta)[:1])
        rows.append(jnp.zeros((8 - 2 * heads, half_rows), F32))
        out_ref[half] = jnp.concatenate(rows, axis=0)
    for slot in range(1, LINE):
        copies[slot - 1].wait_recv()
        rows_ref[:, :, slot * width:(slot + 1) * width] = o_buf[slot - 1]
    for copy in copies:
        copy.wait_send()


def backward_kernel(n_sh, heads, dim, q_ref, do_ref, st_ref, all_ref, dq_ref, dkv_ref,
                    kv_buf, q_buf, do_buf, st_buf, acc_ref, lse_ref, dot_ref, dk_acc, dv_acc, sends, recvs, sems):
    rank, rank_of, barrier, start, wait_recv, wait_sends = shard_exchange(
        n_sh, [(q_ref, q_buf), (do_ref, do_buf), (st_ref, st_buf)], sends, recvs)
    n_x = n_sh // 2
    barrier()
    start("prev", "next", "own_x")
    load = [pltpu.make_async_copy(all_ref, kv_buf, sems.at[0])]
    for idx, (own, buf) in enumerate([(q_ref, q_buf), (do_ref, do_buf), (st_ref, st_buf)]):
        load.append(pltpu.make_async_copy(own, buf.at[pl.ds(2 * rank, 2)], sems.at[1 + idx]))
    for copy in load:
        copy.start()
    width = heads * dim
    half_rows = q_ref.shape[1]
    scale = dim ** -0.5
    log2e_scale = math.log2(math.e) * scale
    for half in range(2):
        for h in range(heads):
            lse_ref[half, h] = jnp.transpose(jnp.broadcast_to(st_ref[half, h:h + 1, :], (dim, half_rows)))
            dot_ref[half, h] = jnp.transpose(jnp.broadcast_to(st_ref[half, heads + h:heads + h + 1, :], (dim, half_rows)))
    for copy in load:
        copy.wait()

    def query_part(half, slot, h, masked):
        cols = slice(h * dim, (h + 1) * dim)
        vcols = slice(width + h * dim, width + (h + 1) * dim)
        k_blk = kv_buf[slot, :, cols]
        v_blk = kv_buf[slot, :, vcols]
        s = dot_t(q_ref[half, :, cols], k_blk)
        p = jnp.exp2(s * log2e_scale - lse_ref[half, h][:, :1])
        if masked:
            p = jnp.where(causal_mask(half_rows, half_rows), p, 0.0)
        dp = dot_t(do_ref[half, :, cols], v_blk)
        ds = (p * (dp - dot_ref[half, h][:, :1])).astype(BF16)
        return dot_n(ds, k_blk)

    for half in range(2):
        for h in range(heads):
            acc_ref[half, h] = query_part(half, 2 * rank + half, h, True)

    def query_step(t, carry):
        late = (t >= rank).astype(jnp.int32)
        slot = block_slot(t - late * rank, n_sh)
        for h in range(heads):
            acc_ref[late, h] = acc_ref[late, h] + query_part(late, slot, h, False)
        return carry

    lax.fori_loop(0, 2 * n_sh - 1, query_step, 0)
    wait_recv("prev")
    start("far_lo", "prev_x")
    wait_recv("next")
    start("far_hi", "next_x")
    for half in range(2):
        for h in range(heads):
            dq_ref[half, :, h * dim:(h + 1) * dim] = (acc_ref[half, h] * scale).astype(BF16)

    def key_part(half, slot, h, masked):
        cols = slice(h * dim, (h + 1) * dim)
        vcols = slice(width + h * dim, width + (h + 1) * dim)
        q_blk = q_buf[slot, :, cols]
        do_blk = do_buf[slot, :, cols]
        k_slot = 2 * rank + half
        s = dot_t(kv_buf[k_slot, :, cols], q_blk)
        p = jnp.exp2(s * log2e_scale - st_buf[slot, h:h + 1, :])
        if masked:
            p = jnp.where(causal_mask(half_rows, half_rows, transposed=True), p, 0.0)
        dp = dot_t(kv_buf[k_slot, :, vcols], do_blk)
        ds = (p * (dp - st_buf[slot, heads + h:heads + h + 1, :])).astype(BF16)
        return dot_n(ds, q_blk), dot_n(p.astype(BF16), do_blk)

    for half in range(2):
        for h in range(heads):
            dk_acc[half, h], dv_acc[half, h] = key_part(half, 2 * rank + half, h, True)

    offsets = [(0, 0), (0, 1), (n_x - 1, 0), (1, 0), (n_x - 1, 1), (1, 1), (2, 0), (2, 1)]

    def visit(first, count):
        def step(t, carry):
            idx = t // 2
            shard = rank_of(*offsets[0])
            for pos in range(1, n_sh):
                shard = jnp.where(idx == pos, rank_of(*offsets[pos]), shard)
            before = (shard < rank).astype(jnp.int32)
            second = lax.rem(t, 2)
            late = jnp.where(second == 1, before, 0)
            slot = 2 * shard + jnp.where(second == 1, before, 1)
            for h in range(heads):
                dk_part, dv_part = key_part(late, slot, h, False)
                dk_acc[late, h] = dk_acc[late, h] + dk_part
                dv_acc[late, h] = dv_acc[late, h] + dv_part
            return carry
        lax.fori_loop(first, first + count, step, 0)

    visit(0, 1)
    wait_recv("own_x")
    visit(2, 6)
    wait_recv("prev_x", "next_x")
    visit(8, 2)
    wait_recv("far_lo", "far_hi")
    start("far_lo_x", "far_hi_x")
    visit(10, 4)
    wait_recv("far_lo_x", "far_hi_x")
    visit(14, 2)
    for half in range(2):
        for h in range(heads):
            cols = slice(h * dim, (h + 1) * dim)
            vcols = slice(width + h * dim, width + (h + 1) * dim)
            dkv_ref[half, :, cols] = (dk_acc[half, h] * scale).astype(BF16)
            dkv_ref[half, :, vcols] = dv_acc[half, h].astype(BF16)
    wait_sends()


VMEM_SPEC = pl.BlockSpec(memory_space=pltpu.VMEM)
ANY_SPEC = pl.BlockSpec(memory_space=pl.ANY)


def attention_call(kernel, name, collective_id, flops, in_specs, out_specs, out_shape, scratch):
    return pl.pallas_call(
        kernel,
        name=name,
        out_shape=out_shape,
        in_specs=in_specs,
        out_specs=out_specs,
        scratch_shapes=scratch,
        cost_estimate=pl.CostEstimate(flops=flops, bytes_accessed=10 * 2 ** 20, transcendentals=0),
        compiler_params=pltpu.CompilerParams(vmem_limit_bytes=VMEM_LIMIT, collective_id=collective_id, has_side_effects=True),
    )


def solution(mesh):
    n_sh = mesh.shape["cp"]

    def device_fn(x_blk, w_query, w_key, w_value, w_out, dy_blk):
        model_dim, heads, dim = w_query.shape
        width = heads * dim
        wq = w_query.reshape(model_dim, width)
        wkv = jnp.concatenate([w_key.reshape(model_dim, width), w_value.reshape(model_dim, width)], axis=1)
        wo = w_out.reshape(width, model_dim)

        x_rows = lax.all_gather(x_blk, "tp", axis=0, tiled=True)
        dy_rows = lax.all_gather(dy_blk, "tp", axis=0, tiled=True)
        n_rows = x_rows.shape[0]
        half_rows = n_rows // 2
        tile_flops = 4 * (2 * n_sh + 1) * half_rows * half_rows * heads * dim

        kv = dot_n(x_rows, wkv).astype(BF16).reshape(2, half_rows, 2 * width)
        q = dot_n(x_rows, wq).astype(BF16).reshape(2, half_rows, width)
        acc = pltpu.VMEM((2, heads, half_rows, dim), F32)
        dma = pltpu.SemaphoreType.DMA
        kv_all_shape = (2 * n_sh, half_rows, 2 * width)

        o, lse, kv_all, wo_all = attention_call(
            functools.partial(forward_kernel, n_sh, heads, dim), "attn_fwd", 0, 2 * tile_flops,
            [VMEM_SPEC] * 3, [VMEM_SPEC, VMEM_SPEC, ANY_SPEC, ANY_SPEC],
            [jax.ShapeDtypeStruct((2, half_rows, width), BF16), jax.ShapeDtypeStruct((2, heads, half_rows), F32),
             jax.ShapeDtypeStruct(kv_all_shape, BF16), jax.ShapeDtypeStruct((LINE, width, model_dim), BF16)],
            [pltpu.VMEM(kv_all_shape, BF16), acc, acc, acc, dma((9,)), dma((9,)), dma((8,)), dma((8,)), dma((2,))],
        )(q, kv, wo)
        o_flat = o.reshape(n_rows, width)
        d_o = dot_t(dy_rows, wo).astype(BF16).reshape(2, half_rows, width)
        n_z = mesh.shape["tp"] // LINE
        blk_rows = n_rows // mesh.shape["tp"]
        stats, o_rows = pl.pallas_call(
            functools.partial(stats_kernel, heads, dim),
            name="attn_stats",
            out_shape=[jax.ShapeDtypeStruct((2, 8, half_rows), F32), jax.ShapeDtypeStruct((n_z, blk_rows, LINE * width), BF16)],
            in_specs=[VMEM_SPEC] * 3,
            out_specs=[VMEM_SPEC] * 2,
            scratch_shapes=[pltpu.VMEM((LINE - 1, n_z, blk_rows, width), BF16), dma((LINE - 1,)), dma((LINE - 1,))],
            compiler_params=pltpu.CompilerParams(collective_id=2, has_side_effects=True),
        )(o.reshape(n_z, LINE, blk_rows, width), d_o, lse)
        y_part = dot_n(o_rows.reshape(n_z * blk_rows, LINE * width), wo_all.reshape(LINE * width, model_dim))
        y_part, stats = lax.optimization_barrier((y_part, stats))
        columns = [[LINE * z_idx + y_idx for z_idx in range(n_z)] for y_idx in range(LINE)]
        y_blk = lax.psum_scatter(y_part, "tp", scatter_dimension=0, axis_index_groups=columns, tiled=True).astype(BF16)
        shard_buf = pltpu.VMEM((2 * n_sh, half_rows, width), BF16)
        dq, dkv = attention_call(
            functools.partial(backward_kernel, n_sh, heads, dim), "attn_bwd", 1, 7 * tile_flops // 2,
            [VMEM_SPEC, VMEM_SPEC, VMEM_SPEC, ANY_SPEC], [VMEM_SPEC, VMEM_SPEC],
            [jax.ShapeDtypeStruct((2, half_rows, width), BF16), jax.ShapeDtypeStruct((2, half_rows, 2 * width), BF16)],
            [pltpu.VMEM(kv_all_shape, BF16), shard_buf, shard_buf, pltpu.VMEM((2 * n_sh, 8, half_rows), F32),
             acc, acc, acc, acc, acc, dma((27,)), dma((27,)), dma((4,))],
        )(q, d_o, stats, kv_all)

        dq_flat = dq.reshape(n_rows, width)
        dkv_flat = dkv.reshape(n_rows, 2 * width)
        d_all = jnp.concatenate([dq_flat, dkv_flat], axis=1)
        w_all = jnp.concatenate([wq, wkv], axis=1)
        dx_part = dot_t(d_all, w_all)
        dx_blk = lax.psum_scatter(dx_part, "tp", scatter_dimension=0, tiled=True).astype(BF16)

        def weight_grad(lhs, rhs, shape):
            return lax.dot_general(lhs, rhs, ROWS_CONTRACT, preferred_element_type=F32).astype(BF16).reshape(shape)[None]

        grad_wo = weight_grad(o_flat, dy_rows, (heads, dim, model_dim))
        grad_wq = weight_grad(x_rows, dq_flat, (model_dim, heads, dim))
        grad_wk = weight_grad(x_rows, dkv_flat[:, :width], (model_dim, heads, dim))
        grad_wv = weight_grad(x_rows, dkv_flat[:, width:], (model_dim, heads, dim))
        return y_blk, dx_blk, grad_wq, grad_wk, grad_wv, grad_wo

    return jax.shard_map(device_fn, mesh=mesh,
                         in_specs=(ROW_SPEC, HEAD_SPEC, HEAD_SPEC, HEAD_SPEC, OUT_W_SPEC, ROW_SPEC),
                         out_specs=(ROW_SPEC, ROW_SPEC, GRAD_SPEC, GRAD_SPEC, GRAD_SPEC, GRAD_OUT_SPEC),
                         check_vma=False)
```

```python
import functools
import math

import jax
import jax.numpy as jnp
from jax import lax
from jax.experimental import pallas as pl
from jax.experimental.pallas import tpu as pltpu
from jax.sharding import PartitionSpec as P

ROW_SPEC = P(("dp", "cp", "tp"), None)
HEAD_SPEC = P(None, "tp", None)
OUT_W_SPEC = P("tp", None, None)
GRAD_SPEC = P(("dp", "cp"), None, "tp", None)
GRAD_OUT_SPEC = P(("dp", "cp"), "tp", None, None)
COLS_CONTRACT = (((1,), (1,)), ((), ()))
ROWS_CONTRACT = (((0,), (0,)), ((), ()))
VMEM_LIMIT = 58 * 1024 * 1024
F32 = jnp.float32
BF16 = jnp.bfloat16


def dot_t(lhs, rhs):
    return lax.dot_general(lhs, rhs, COLS_CONTRACT, preferred_element_type=F32)


def dot_n(lhs, rhs):
    return jnp.dot(lhs, rhs, preferred_element_type=F32)


LINE = 4


def block_slot(pos_blk, n_sh):
    return jnp.where(pos_blk < n_sh, 2 * pos_blk, 2 * (2 * n_sh - 1 - pos_blk) + 1)


def shard_exchange(n_sh, pairs, sends, recvs):
    n_x = n_sh // 2
    rank = lax.axis_index("cp")
    chip, core = rank // 2, lax.rem(rank, 2)

    def rank_of(dx, dc):
        return 2 * lax.rem(chip + dx, n_x) + lax.rem(core + dc, 2)

    n_kinds = 9
    kinds = {"prev": 0, "next": 1, "far_lo": 2, "far_hi": 3, "own_x": 4, "prev_x": 5, "next_x": 6, "far_lo_x": 7, "far_hi_x": 8}

    def part(buf, dx, dc, half):
        return buf.at[pl.ds(2 * rank_of(dx, dc) + (0 if half is None else half), 2 if half is None else 1)]

    routes = {
        "prev": ((0, 0), None, (1, 0)), "next": ((0, 0), None, (n_x - 1, 0)), "own_x": ((0, 0), None, (0, 1)),
        "far_lo": ((n_x - 1, 0), 0, (1, 0)), "far_hi": ((1, 0), 1, (n_x - 1, 0)),
        "prev_x": ((n_x - 1, 0), None, (0, 1)), "next_x": ((1, 0), None, (0, 1)),
        "far_lo_x": ((2, 0), 0, (0, 1)), "far_hi_x": ((2, 0), 1, (0, 1)),
    }

    def copies(kind):
        (dx, dc), half, target = routes[kind]
        out = []
        for idx, (own, buf) in enumerate(pairs):
            dst = part(buf, dx, dc, half)
            src = own if (dx, dc) == (0, 0) else dst
            out.append(pltpu.make_async_remote_copy(
                src_ref=src, dst_ref=dst, send_sem=sends.at[idx * n_kinds + kinds[kind]], recv_sem=recvs.at[idx * n_kinds + kinds[kind]],
                device_id={"cp": rank_of(*target)}, device_id_type=pl.DeviceIdType.MESH))
        return out

    def start(*names):
        for name in names:
            for copy in copies(name):
                copy.start()

    def wait_recv(*names):
        for name in names:
            for copy in copies(name):
                copy.wait_recv()

    def wait_sends():
        for name in routes:
            for copy in copies(name):
                copy.wait_send()

    def barrier(others=()):
        sem = pltpu.get_barrier_semaphore()
        for target in [{"cp": rank_of(*offset)} for offset in ((1, 0), (n_x - 1, 0), (0, 1))] + list(others):
            pl.semaphore_signal(sem, inc=1, device_id=target, device_id_type=pl.DeviceIdType.MESH)
        pl.semaphore_wait(sem, 3 + len(others))

    return rank, rank_of, barrier, start, wait_recv, wait_sends


def line_device(shift):
    tp_idx = lax.axis_index("tp")
    return {"tp": LINE * (tp_idx // LINE) + lax.rem(lax.rem(tp_idx, LINE) + shift + LINE, LINE)}


def weight_gather(w_ref, slot_ref, other_core, sends, recvs):
    core = lax.rem(lax.axis_index("cp"), 2)
    part_rows = w_ref.shape[0] // 2
    quarter = part_rows // 2
    first = core * part_rows

    def whole(slot):
        return slot_ref(slot).at[pl.ds(first, part_rows)]

    def lo(slot):
        return slot_ref(slot).at[pl.ds(first, quarter)]

    def hi(slot):
        return slot_ref(slot).at[pl.ds(first + quarter, quarter)]

    own = w_ref.at[pl.ds(first, part_rows)]
    routes = [
        ("prev", own, whole(1), line_device(1)), ("next", own, whole(2), line_device(-1)),
        ("far_lo", lo(1), lo(3), line_device(1)), ("far_hi", hi(2), hi(3), line_device(-1)),
        ("prev_x", whole(1), whole(1), other_core), ("next_x", whole(2), whole(2), other_core),
        ("far_lo_x", lo(3), lo(3), other_core), ("far_hi_x", hi(3), hi(3), other_core),
    ]

    def copy_of(name):
        for idx, (kind, src, dst, target) in enumerate(routes):
            if kind == name:
                return pltpu.make_async_remote_copy(src_ref=src, dst_ref=dst, send_sem=sends.at[idx], recv_sem=recvs.at[idx],
                                                    device_id=target, device_id_type=pl.DeviceIdType.MESH)

    def start(*names):
        for name in names:
            copy_of(name).start()

    def wait_recv(*names):
        for name in names:
            copy_of(name).wait_recv()

    def wait_sends():
        for route in routes:
            copy_of(route[0]).wait_send()

    return start, wait_recv, wait_sends


def causal_mask(rows, cols, transposed=False):
    row_ids = lax.broadcasted_iota(jnp.int32, (rows, cols), 0)
    col_ids = lax.broadcasted_iota(jnp.int32, (rows, cols), 1)
    return col_ids >= row_ids if transposed else row_ids >= col_ids


def forward_kernel(n_sh, heads, dim, q_ref, kv_ref, wo_ref, o_ref, lse_ref, all_ref, wo_all_ref,
                   kv_buf, m_ref, l_ref, acc_ref, sends, recvs, w_sends, w_recvs, sems):
    rank, rank_of, barrier, start, wait_recv, wait_sends = shard_exchange(n_sh, [(kv_ref, kv_buf)], sends, recvs)
    n_x = n_sh // 2
    w_start, w_wait, w_wait_sends = weight_gather(wo_ref, lambda slot: wo_all_ref.at[slot], {"cp": rank_of(0, 1)}, w_sends, w_recvs)
    barrier([line_device(1), line_device(-1)])
    start("prev", "next", "own_x")
    w_start("prev", "next")
    width = heads * dim
    half_rows = q_ref.shape[1]
    log2e_scale = math.log2(math.e) * dim ** -0.5
    own_w = pltpu.make_async_copy(wo_ref, wo_all_ref.at[0], sems.at[1])
    own_w.start()
    own = pltpu.make_async_copy(kv_ref, kv_buf.at[pl.ds(2 * rank, 2)], sems.at[0])
    own.start()
    own.wait()
    for half in range(2):
        for h in range(heads):
            cols = slice(h * dim, (h + 1) * dim)
            vcols = slice(width + h * dim, width + (h + 1) * dim)
            k_blk = kv_buf[2 * rank + half, :, cols]
            v_blk = kv_buf[2 * rank + half, :, vcols]
            s = dot_t(q_ref[half, :, cols], k_blk)
            s = jnp.where(causal_mask(half_rows, half_rows), s, -jnp.inf)
            m = jnp.max(s, axis=1, keepdims=True)
            p = jnp.exp2((s - m) * log2e_scale)
            m_ref[half, h] = jnp.broadcast_to(m, (half_rows, dim))
            l_ref[half, h] = jnp.broadcast_to(jnp.sum(p, axis=1, keepdims=True), (half_rows, dim))
            acc_ref[half, h] = dot_n(p.astype(BF16), v_blk)

    def unit(late, slot):
        for h in range(heads):
            cols = slice(h * dim, (h + 1) * dim)
            vcols = slice(width + h * dim, width + (h + 1) * dim)
            k_blk = kv_buf[slot, :, cols]
            v_blk = kv_buf[slot, :, vcols]
            s = dot_t(q_ref[late, :, cols], k_blk)
            m_old = m_ref[late, h]
            m_new = jnp.maximum(m_old, jnp.max(s, axis=1, keepdims=True))
            factor = jnp.exp2((m_old - m_new) * log2e_scale)
            p = jnp.exp2((s - m_new[:, :1]) * log2e_scale)
            m_ref[late, h] = m_new
            l_ref[late, h] = l_ref[late, h] * factor + jnp.sum(p, axis=1, keepdims=True)
            acc_ref[late, h] = acc_ref[late, h] * factor + dot_n(p.astype(BF16), v_blk)

    def visit(first, count, shard_of):
        def step(t, carry):
            shard = shard_of(t // 2)
            after = (shard > rank).astype(jnp.int32)
            second = lax.rem(t, 2)
            late = jnp.where(second == 1, after, 1)
            slot = 2 * shard + jnp.where(second == 1, after, 0)
            unit(late, slot)
            return carry
        lax.fori_loop(first, first + count, step, 0)

    offsets = [(0, 0), (0, 1), (n_x - 1, 0), (1, 0), (n_x - 1, 1), (1, 1), (2, 0), (2, 1)]

    def shard_of(idx):
        out = rank_of(*offsets[0])
        for pos in range(1, n_sh):
            out = jnp.where(idx == pos, rank_of(*offsets[pos]), out)
        return out

    visit(0, 1, shard_of)
    wait_recv("own_x")
    visit(2, 2, shard_of)
    wait_recv("prev")
    start("far_lo", "prev_x")
    wait_recv("next")
    start("far_hi", "next_x")
    visit(4, 4, shard_of)
    w_wait("prev")
    w_start("far_lo", "prev_x")
    w_wait("next")
    w_start("far_hi", "next_x")
    wait_recv("prev_x", "next_x")
    visit(8, 2, shard_of)
    wait_recv("far_lo", "far_hi")
    start("far_lo_x", "far_hi_x")
    visit(10, 4, shard_of)
    wait_recv("far_lo_x", "far_hi_x")
    out = pltpu.make_async_copy(kv_buf, all_ref, sems.at[0])
    out.start()
    visit(14, 2, shard_of)
    w_wait("far_lo", "far_hi")
    w_start("far_lo_x", "far_hi_x")
    for half in range(2):
        for h in range(heads):
            cols = slice(h * dim, (h + 1) * dim)
            l = l_ref[half, h]
            o_ref[half, :, cols] = (acc_ref[half, h] / l).astype(BF16)
            lse = m_ref[half, h] * log2e_scale + jnp.log2(l)
            lse_ref[half, h:h + 1, :] = jnp.transpose(lse)[:1]
    out.wait()
    own_w.wait()
    w_wait("prev_x", "next_x", "far_lo_x", "far_hi_x")
    wait_sends()
    w_wait_sends()


def stats_kernel(heads, dim, o_ref, do_ref, lse_ref, out_ref, rows_ref, o_buf, sends, recvs):
    y_pos = lax.rem(lax.axis_index("tp"), LINE)
    shifts = (0, 1, -1, 2)
    sem = pltpu.get_barrier_semaphore()
    for shift in shifts[1:]:
        pl.semaphore_signal(sem, inc=1, device_id=line_device(shift), device_id_type=pl.DeviceIdType.MESH)
    pl.semaphore_wait(sem, 3)
    copies = []
    for slot in range(1, LINE):
        target = line_device(shifts[slot])
        copies.append(pltpu.make_async_remote_copy(
            src_ref=o_ref.at[:, lax.rem(target["tp"], LINE)], dst_ref=o_buf.at[slot - 1], send_sem=sends.at[slot - 1],
            recv_sem=recvs.at[slot - 1], device_id=target, device_id_type=pl.DeviceIdType.MESH))
        copies[-1].start()
    width = heads * dim
    rows_ref[:, :, :width] = o_ref[:, y_pos]
    half_rows = lse_ref.shape[2]
    o_rows = o_ref[...].reshape(2, half_rows, width)
    for half in range(2):
        rows = [lse_ref[half]]
        for h in range(heads):
            cols = slice(h * dim, (h + 1) * dim)
            prod = do_ref[half, :, cols].astype(F32) * o_rows[half, :, cols].astype(F32)
            delta = jnp.broadcast_to(jnp.sum(prod, axis=1, keepdims=True), (half_rows, dim))
            rows.append(jnp.transpose(delta)[:1])
        rows.append(jnp.zeros((8 - 2 * heads, half_rows), F32))
        out_ref[half] = jnp.concatenate(rows, axis=0)
    for slot in range(1, LINE):
        copies[slot - 1].wait_recv()
        rows_ref[:, :, slot * width:(slot + 1) * width] = o_buf[slot - 1]
    for copy in copies:
        copy.wait_send()


def backward_kernel(n_sh, heads, dim, q_ref, do_ref, st_ref, all_ref, w_ref, dq_ref, dkv_ref, w_prev_ref, w_next_ref, w_far_ref,
                    kv_buf, q_buf, do_buf, st_buf, acc_ref, lse_ref, dot_ref, dk_acc, dv_acc, sends, recvs, w_sends, w_recvs, sems):
    rank, rank_of, barrier, start, wait_recv, wait_sends = shard_exchange(
        n_sh, [(q_ref, q_buf), (do_ref, do_buf), (st_ref, st_buf)], sends, recvs)
    n_x = n_sh // 2
    w_slots = (None, w_prev_ref, w_next_ref, w_far_ref)
    w_start, w_wait, w_wait_sends = weight_gather(w_ref, lambda slot: w_slots[slot], {"cp": rank_of(0, 1)}, w_sends, w_recvs)
    barrier([line_device(1), line_device(-1)])
    start("prev", "next", "own_x")
    w_start("prev", "next")
    load = [pltpu.make_async_copy(all_ref, kv_buf, sems.at[0])]
    for idx, (own, buf) in enumerate([(q_ref, q_buf), (do_ref, do_buf), (st_ref, st_buf)]):
        load.append(pltpu.make_async_copy(own, buf.at[pl.ds(2 * rank, 2)], sems.at[1 + idx]))
    for copy in load:
        copy.start()
    width = heads * dim
    half_rows = q_ref.shape[1]
    scale = dim ** -0.5
    log2e_scale = math.log2(math.e) * scale
    for half in range(2):
        for h in range(heads):
            lse_ref[half, h] = jnp.transpose(jnp.broadcast_to(st_ref[half, h:h + 1, :], (dim, half_rows)))
            dot_ref[half, h] = jnp.transpose(jnp.broadcast_to(st_ref[half, heads + h:heads + h + 1, :], (dim, half_rows)))
    for copy in load:
        copy.wait()

    def query_part(half, slot, h, masked):
        cols = slice(h * dim, (h + 1) * dim)
        vcols = slice(width + h * dim, width + (h + 1) * dim)
        k_blk = kv_buf[slot, :, cols]
        v_blk = kv_buf[slot, :, vcols]
        s = dot_t(q_ref[half, :, cols], k_blk)
        p = jnp.exp2(s * log2e_scale - lse_ref[half, h][:, :1])
        if masked:
            p = jnp.where(causal_mask(half_rows, half_rows), p, 0.0)
        dp = dot_t(do_ref[half, :, cols], v_blk)
        ds = (p * (dp - dot_ref[half, h][:, :1])).astype(BF16)
        return dot_n(ds, k_blk)

    for half in range(2):
        for h in range(heads):
            acc_ref[half, h] = query_part(half, 2 * rank + half, h, True)

    def query_step(t, carry):
        late = (t >= rank).astype(jnp.int32)
        slot = block_slot(t - late * rank, n_sh)
        for h in range(heads):
            acc_ref[late, h] = acc_ref[late, h] + query_part(late, slot, h, False)
        return carry

    lax.fori_loop(0, 2 * n_sh - 1, query_step, 0)
    wait_recv("prev")
    start("far_lo", "prev_x")
    wait_recv("next")
    start("far_hi", "next_x")
    for half in range(2):
        for h in range(heads):
            dq_ref[half, :, h * dim:(h + 1) * dim] = (acc_ref[half, h] * scale).astype(BF16)

    def key_part(half, slot, h, masked):
        cols = slice(h * dim, (h + 1) * dim)
        vcols = slice(width + h * dim, width + (h + 1) * dim)
        q_blk = q_buf[slot, :, cols]
        do_blk = do_buf[slot, :, cols]
        k_slot = 2 * rank + half
        s = dot_t(kv_buf[k_slot, :, cols], q_blk)
        p = jnp.exp2(s * log2e_scale - st_buf[slot, h:h + 1, :])
        if masked:
            p = jnp.where(causal_mask(half_rows, half_rows, transposed=True), p, 0.0)
        dp = dot_t(kv_buf[k_slot, :, vcols], do_blk)
        ds = (p * (dp - st_buf[slot, heads + h:heads + h + 1, :])).astype(BF16)
        return dot_n(ds, q_blk), dot_n(p.astype(BF16), do_blk)

    for half in range(2):
        for h in range(heads):
            dk_acc[half, h], dv_acc[half, h] = key_part(half, 2 * rank + half, h, True)

    offsets = [(0, 0), (0, 1), (n_x - 1, 0), (1, 0), (n_x - 1, 1), (1, 1), (2, 0), (2, 1)]

    def visit(first, count):
        def step(t, carry):
            idx = t // 2
            shard = rank_of(*offsets[0])
            for pos in range(1, n_sh):
                shard = jnp.where(idx == pos, rank_of(*offsets[pos]), shard)
            before = (shard < rank).astype(jnp.int32)
            second = lax.rem(t, 2)
            late = jnp.where(second == 1, before, 0)
            slot = 2 * shard + jnp.where(second == 1, before, 1)
            for h in range(heads):
                dk_part, dv_part = key_part(late, slot, h, False)
                dk_acc[late, h] = dk_acc[late, h] + dk_part
                dv_acc[late, h] = dv_acc[late, h] + dv_part
            return carry
        lax.fori_loop(first, first + count, step, 0)

    visit(0, 1)
    wait_recv("own_x")
    visit(2, 2)
    w_wait("prev")
    w_start("far_lo", "prev_x")
    w_wait("next")
    w_start("far_hi", "next_x")
    visit(4, 4)
    wait_recv("prev_x", "next_x")
    visit(8, 2)
    wait_recv("far_lo", "far_hi")
    start("far_lo_x", "far_hi_x")
    visit(10, 4)
    wait_recv("far_lo_x", "far_hi_x")
    visit(14, 2)
    w_wait("far_lo", "far_hi")
    w_start("far_lo_x", "far_hi_x")
    for half in range(2):
        for h in range(heads):
            cols = slice(h * dim, (h + 1) * dim)
            vcols = slice(width + h * dim, width + (h + 1) * dim)
            dkv_ref[half, :, cols] = (dk_acc[half, h] * scale).astype(BF16)
            dkv_ref[half, :, vcols] = dv_acc[half, h].astype(BF16)
    w_wait("prev_x", "next_x", "far_lo_x", "far_hi_x")
    wait_sends()
    w_wait_sends()


def grad_rows_kernel(dq_ref, dkv_ref, own_ref, prev_ref, next_ref, far_ref, dq_buf, dkv_buf, sends, recvs):
    y_pos = lax.rem(lax.axis_index("tp"), LINE)
    shifts = (0, 1, -1, 2)
    sem = pltpu.get_barrier_semaphore()
    for shift in shifts[1:]:
        pl.semaphore_signal(sem, inc=1, device_id=line_device(shift), device_id_type=pl.DeviceIdType.MESH)
    pl.semaphore_wait(sem, LINE - 1)
    copies = []
    for slot in range(1, LINE):
        target = line_device(shifts[slot])
        for idx, (src, buf) in enumerate([(dq_ref, dq_buf), (dkv_ref, dkv_buf)]):
            copies.append(pltpu.make_async_remote_copy(
                src_ref=src.at[:, lax.rem(target["tp"], LINE)], dst_ref=buf.at[slot - 1], send_sem=sends.at[2 * slot - 2 + idx],
                recv_sem=recvs.at[2 * slot - 2 + idx], device_id=target, device_id_type=pl.DeviceIdType.MESH))
            copies[-1].start()
    width = dq_ref.shape[3]
    own_ref[:, :, :width] = dq_ref[:, y_pos]
    own_ref[:, :, width:] = dkv_ref[:, y_pos]
    for copy in copies:
        copy.wait_recv()
    for slot, out_ref in enumerate((prev_ref, next_ref, far_ref)):
        out_ref[:, :, :width] = dq_buf[slot]
        out_ref[:, :, width:] = dkv_buf[slot]
    for copy in copies:
        copy.wait_send()


def gather_rows_kernel(x_ref, all_ref, sends, recvs, sem):
    tp_idx = lax.axis_index("tp")
    pos = (tp_idx // LINE, lax.rem(tp_idx, LINE))
    half_rows = x_ref.shape[0] // 2
    quarter = half_rows // 2

    def block(axis, fast, slow):
        off = (slow, fast) if axis == 1 else (fast, slow)
        z_idx, y_idx = [lax.rem(base + shift + LINE, LINE) for base, shift in zip(pos, off)]
        return LINE * z_idx + y_idx

    barrier = pltpu.get_barrier_semaphore()
    for axis in range(2):
        for shift in (1, -1):
            pl.semaphore_signal(barrier, inc=1, device_id={"tp": block(axis, shift, 0)}, device_id_type=pl.DeviceIdType.MESH)
    pl.semaphore_wait(barrier, 4)

    own = pltpu.make_async_copy(x_ref, all_ref.at[block(1, 0, 0)], sem.at[0])
    own.start()
    table = {}
    for colour in range(2):
        axis = 1 - colour
        base = colour * half_rows
        whole, low, high = (base, half_rows), (base, quarter), (base + quarter, quarter)

        def add(name, fast, slow, rows, along_fast, shift):
            idx = len(table)
            span = pl.ds(*rows)
            blk = block(axis, fast, slow)
            src = x_ref.at[span] if fast == 0 and slow == 0 else all_ref.at[blk, span]
            target = block(axis, shift, 0) if along_fast else block(axis, 0, shift)
            table[colour, name] = pltpu.make_async_remote_copy(
                src_ref=src, dst_ref=all_ref.at[blk, span], send_sem=sends.at[idx], recv_sem=recvs.at[idx],
                device_id={"tp": target}, device_id_type=pl.DeviceIdType.MESH)

        add("prev", 0, 0, whole, True, 1)
        add("next", 0, 0, whole, True, -1)
        add("far_lo", -1, 0, low, True, 1)
        add("far_hi", 1, 0, high, True, -1)
        for fast in (0, -1, 1, 2):
            add(("prev", fast), fast, 0, whole, False, 1)
            add(("next", fast), fast, 0, whole, False, -1)
            add(("far_lo", fast), fast, -1, low, False, 1)
            add(("far_hi", fast), fast, 1, high, False, -1)

    def start(*names):
        for name in names:
            for colour in range(2):
                table[colour, name].start()

    def wait(*names):
        for name in names:
            for colour in range(2):
                table[colour, name].wait_recv()

    start("prev", "next", ("prev", 0), ("next", 0))
    wait("prev")
    start("far_lo", ("prev", -1), ("next", -1))
    wait("next")
    start("far_hi", ("prev", 1), ("next", 1))
    wait(("prev", 0))
    start(("far_lo", 0))
    wait(("next", 0))
    start(("far_hi", 0))
    wait("far_lo", "far_hi")
    start(("prev", 2), ("next", 2))
    for fast in (-1, 1, 2):
        wait(("prev", fast))
        start(("far_lo", fast))
        wait(("next", fast))
        start(("far_hi", fast))
    for fast in (0, -1, 1, 2):
        wait(("far_lo", fast), ("far_hi", fast))
    own.wait()
    for copy in table.values():
        copy.wait_send()


def gather_rows(x_blk, n_tp):
    rows, cols = x_blk.shape
    if n_tp != LINE * LINE:
        return lax.all_gather(x_blk, "tp", axis=0, tiled=True)
    gathered = pl.pallas_call(
        gather_rows_kernel,
        name="gather_rows",
        out_shape=jax.ShapeDtypeStruct((n_tp, rows, cols), x_blk.dtype),
        in_specs=[VMEM_SPEC],
        out_specs=ANY_SPEC,
        scratch_shapes=[pltpu.SemaphoreType.DMA((40,)), pltpu.SemaphoreType.DMA((40,)), pltpu.SemaphoreType.DMA((1,))],
        compiler_params=pltpu.CompilerParams(collective_id=4, has_side_effects=True),
    )(x_blk)
    return gathered.reshape(n_tp * rows, cols)


VMEM_SPEC = pl.BlockSpec(memory_space=pltpu.VMEM)
ANY_SPEC = pl.BlockSpec(memory_space=pl.ANY)


def attention_call(kernel, name, collective_id, flops, in_specs, out_specs, out_shape, scratch):
    return pl.pallas_call(
        kernel,
        name=name,
        out_shape=out_shape,
        in_specs=in_specs,
        out_specs=out_specs,
        scratch_shapes=scratch,
        cost_estimate=pl.CostEstimate(flops=flops, bytes_accessed=10 * 2 ** 20, transcendentals=0),
        compiler_params=pltpu.CompilerParams(vmem_limit_bytes=VMEM_LIMIT, collective_id=collective_id, has_side_effects=True),
    )


def solution(mesh):
    n_sh = mesh.shape["cp"]

    def device_fn(x_blk, w_query, w_key, w_value, w_out, dy_blk):
        model_dim, heads, dim = w_query.shape
        width = heads * dim
        wq = w_query.reshape(model_dim, width)
        wkv = jnp.concatenate([w_key.reshape(model_dim, width), w_value.reshape(model_dim, width)], axis=1)
        wo = w_out.reshape(width, model_dim)

        x_rows = gather_rows(x_blk, mesh.shape["tp"])
        x_rows, dy_blk = lax.optimization_barrier((x_rows, dy_blk))
        dy_rows = lax.all_gather(dy_blk, "tp", axis=0, tiled=True)
        n_rows = x_rows.shape[0]
        half_rows = n_rows // 2
        tile_flops = 4 * (2 * n_sh + 1) * half_rows * half_rows * heads * dim

        kv = dot_n(x_rows, wkv).astype(BF16).reshape(2, half_rows, 2 * width)
        q = dot_n(x_rows, wq).astype(BF16).reshape(2, half_rows, width)
        acc = pltpu.VMEM((2, heads, half_rows, dim), F32)
        dma = pltpu.SemaphoreType.DMA
        kv_all_shape = (2 * n_sh, half_rows, 2 * width)

        o, lse, kv_all, wo_all = attention_call(
            functools.partial(forward_kernel, n_sh, heads, dim), "attn_fwd", 0, 2 * tile_flops,
            [VMEM_SPEC] * 3, [VMEM_SPEC, VMEM_SPEC, ANY_SPEC, ANY_SPEC],
            [jax.ShapeDtypeStruct((2, half_rows, width), BF16), jax.ShapeDtypeStruct((2, heads, half_rows), F32),
             jax.ShapeDtypeStruct(kv_all_shape, BF16), jax.ShapeDtypeStruct((LINE, width, model_dim), BF16)],
            [pltpu.VMEM(kv_all_shape, BF16), acc, acc, acc, dma((9,)), dma((9,)), dma((8,)), dma((8,)), dma((2,))],
        )(q, kv, wo)
        o_flat = o.reshape(n_rows, width)
        lse, *late_weights = lax.optimization_barrier((lse, w_query, w_key, w_value))
        w_all = jnp.concatenate([w_late.reshape(model_dim, width) for w_late in late_weights], axis=1)
        n_cols = model_dim // 2
        w_shared = w_all[n_cols:]
        d_o = dot_t(dy_rows, wo).astype(BF16).reshape(2, half_rows, width)
        n_z = mesh.shape["tp"] // LINE
        blk_rows = n_rows // mesh.shape["tp"]
        stats, o_rows = pl.pallas_call(
            functools.partial(stats_kernel, heads, dim),
            name="attn_stats",
            out_shape=[jax.ShapeDtypeStruct((2, 8, half_rows), F32), jax.ShapeDtypeStruct((n_z, blk_rows, LINE * width), BF16)],
            in_specs=[VMEM_SPEC] * 3,
            out_specs=[VMEM_SPEC] * 2,
            scratch_shapes=[pltpu.VMEM((LINE - 1, n_z, blk_rows, width), BF16), dma((LINE - 1,)), dma((LINE - 1,))],
            compiler_params=pltpu.CompilerParams(collective_id=2, has_side_effects=True),
        )(o.reshape(n_z, LINE, blk_rows, width), d_o, lse)
        y_part = dot_n(o_rows.reshape(n_z * blk_rows, LINE * width), wo_all.reshape(LINE * width, model_dim))
        y_part, stats = lax.optimization_barrier((y_part, stats))
        columns = [[LINE * z_idx + y_idx for z_idx in range(n_z)] for y_idx in range(LINE)]
        y_sum = lax.psum_scatter(y_part, "tp", scatter_dimension=0, axis_index_groups=columns, tiled=True)
        shard_buf = pltpu.VMEM((2 * n_sh, half_rows, width), BF16)
        w_slot = jax.ShapeDtypeStruct(w_shared.shape, BF16)
        dq, dkv, w_prev, w_next, w_far = attention_call(
            functools.partial(backward_kernel, n_sh, heads, dim), "attn_bwd", 1, 7 * tile_flops // 2,
            [VMEM_SPEC, VMEM_SPEC, VMEM_SPEC, ANY_SPEC, ANY_SPEC], [VMEM_SPEC, VMEM_SPEC] + [ANY_SPEC] * 3,
            [jax.ShapeDtypeStruct((2, half_rows, width), BF16), jax.ShapeDtypeStruct((2, half_rows, 2 * width), BF16)] + [w_slot] * 3,
            [pltpu.VMEM(kv_all_shape, BF16), shard_buf, shard_buf, pltpu.VMEM((2 * n_sh, 8, half_rows), F32),
             acc, acc, acc, acc, acc, dma((27,)), dma((27,)), dma((8,)), dma((8,)), dma((4,))],
        )(q, d_o, stats, kv_all, w_shared)

        dq_flat = dq.reshape(n_rows, width)
        dkv_flat = dkv.reshape(n_rows, 2 * width)
        d_all = jnp.concatenate([dq_flat, dkv_flat], axis=1)
        dx_first = dot_t(d_all, w_all[:n_cols])
        dx_first, dq, dkv, y_sum = lax.optimization_barrier((dx_first, dq, dkv, y_sum))
        dx_first = lax.psum_scatter(dx_first, "tp", scatter_dimension=0, tiled=True)
        d_rows = pl.pallas_call(
            grad_rows_kernel,
            name="grad_rows",
            out_shape=[jax.ShapeDtypeStruct((n_z, blk_rows, 3 * width), BF16)] * LINE,
            in_specs=[VMEM_SPEC] * 2,
            out_specs=[VMEM_SPEC] * LINE,
            scratch_shapes=[pltpu.VMEM((LINE - 1, n_z, blk_rows, width), BF16), pltpu.VMEM((LINE - 1, n_z, blk_rows, 2 * width), BF16),
                            dma((2 * LINE - 2,)), dma((2 * LINE - 2,))],
            compiler_params=pltpu.CompilerParams(collective_id=3, has_side_effects=True),
        )(dq.reshape(n_z, LINE, blk_rows, width), dkv.reshape(n_z, LINE, blk_rows, 2 * width))
        d_rows = [part.reshape(n_z * blk_rows, 3 * width) for part in d_rows]
        dx_second = dot_t(d_rows[0], w_shared)
        for slot, w_part in enumerate((w_prev, w_next, w_far)):
            dx_second = dx_second + dot_t(d_rows[slot + 1], w_part)
        dq_flat = dq.reshape(n_rows, width)
        dkv_flat = dkv.reshape(n_rows, 2 * width)

        def weight_grad(lhs, rhs, shape):
            return lax.dot_general(lhs, rhs, ROWS_CONTRACT, preferred_element_type=F32).astype(BF16).reshape(shape)[None]

        grad_wo = weight_grad(o_flat, dy_rows, (heads, dim, model_dim))
        grad_wq = weight_grad(x_rows, dq_flat, (model_dim, heads, dim))
        grad_wk = weight_grad(x_rows, dkv_flat[:, :width], (model_dim, heads, dim))
        grad_wv = weight_grad(x_rows, dkv_flat[:, width:], (model_dim, heads, dim))
        dx_second, dx_first, grad_wo, grad_wq, grad_wk = lax.optimization_barrier((dx_second, dx_first, grad_wo, grad_wq, grad_wk))
        dx_second = lax.psum_scatter(dx_second, "tp", scatter_dimension=0, axis_index_groups=columns, tiled=True)
        dx_blk = jnp.concatenate([dx_first, dx_second], axis=1).astype(BF16)
        return y_sum.astype(BF16), dx_blk, grad_wq, grad_wk, grad_wv, grad_wo

    return jax.shard_map(device_fn, mesh=mesh,
                         in_specs=(ROW_SPEC, HEAD_SPEC, HEAD_SPEC, HEAD_SPEC, OUT_W_SPEC, ROW_SPEC),
                         out_specs=(ROW_SPEC, ROW_SPEC, GRAD_SPEC, GRAD_SPEC, GRAD_SPEC, GRAD_OUT_SPEC),
                         check_vma=False)
```

```python
import functools
import math

import jax
import jax.numpy as jnp
from jax import lax
from jax.experimental import pallas as pl
from jax.experimental.pallas import tpu as pltpu
from jax.sharding import PartitionSpec as P

ROW_SPEC = P(("dp", "cp", "tp"), None)
HEAD_SPEC = P(None, "tp", None)
OUT_W_SPEC = P("tp", None, None)
GRAD_SPEC = P(("dp", "cp"), None, "tp", None)
GRAD_OUT_SPEC = P(("dp", "cp"), "tp", None, None)
COLS_CONTRACT = (((1,), (1,)), ((), ()))
ROWS_CONTRACT = (((0,), (0,)), ((), ()))
VMEM_LIMIT = 58 * 1024 * 1024
F32 = jnp.float32
BF16 = jnp.bfloat16


def dot_t(lhs, rhs):
    return lax.dot_general(lhs, rhs, COLS_CONTRACT, preferred_element_type=F32)


def dot_n(lhs, rhs):
    return jnp.dot(lhs, rhs, preferred_element_type=F32)


LINE = 4


def block_slot(pos_blk, n_sh):
    return jnp.where(pos_blk < n_sh, 2 * pos_blk, 2 * (2 * n_sh - 1 - pos_blk) + 1)


def shard_exchange(n_sh, pairs, sends, recvs):
    n_x = n_sh // 2
    rank = lax.axis_index("cp")
    chip, core = rank // 2, lax.rem(rank, 2)

    def rank_of(dx, dc):
        return 2 * lax.rem(chip + dx, n_x) + lax.rem(core + dc, 2)

    n_kinds = 9
    kinds = {"prev": 0, "next": 1, "far_lo": 2, "far_hi": 3, "own_x": 4, "prev_x": 5, "next_x": 6, "far_lo_x": 7, "far_hi_x": 8}

    def part(buf, dx, dc, half):
        return buf.at[pl.ds(2 * rank_of(dx, dc) + (0 if half is None else half), 2 if half is None else 1)]

    routes = {
        "prev": ((0, 0), None, (1, 0)), "next": ((0, 0), None, (n_x - 1, 0)), "own_x": ((0, 0), None, (0, 1)),
        "far_lo": ((n_x - 1, 0), 0, (1, 0)), "far_hi": ((1, 0), 1, (n_x - 1, 0)),
        "prev_x": ((n_x - 1, 0), None, (0, 1)), "next_x": ((1, 0), None, (0, 1)),
        "far_lo_x": ((2, 0), 0, (0, 1)), "far_hi_x": ((2, 0), 1, (0, 1)),
    }

    def copies(kind):
        (dx, dc), half, target = routes[kind]
        out = []
        for idx, (own, buf) in enumerate(pairs):
            dst = part(buf, dx, dc, half)
            src = own if (dx, dc) == (0, 0) else dst
            out.append(pltpu.make_async_remote_copy(
                src_ref=src, dst_ref=dst, send_sem=sends.at[idx * n_kinds + kinds[kind]], recv_sem=recvs.at[idx * n_kinds + kinds[kind]],
                device_id={"cp": rank_of(*target)}, device_id_type=pl.DeviceIdType.MESH))
        return out

    def start(*names):
        for name in names:
            for copy in copies(name):
                copy.start()

    def wait_recv(*names):
        for name in names:
            for copy in copies(name):
                copy.wait_recv()

    def wait_sends():
        for name in routes:
            for copy in copies(name):
                copy.wait_send()

    def barrier(others=()):
        sem = pltpu.get_barrier_semaphore()
        for target in [{"cp": rank_of(*offset)} for offset in ((1, 0), (n_x - 1, 0), (0, 1))] + list(others):
            pl.semaphore_signal(sem, inc=1, device_id=target, device_id_type=pl.DeviceIdType.MESH)
        pl.semaphore_wait(sem, 3 + len(others))

    return rank, rank_of, barrier, start, wait_recv, wait_sends


def line_device(shift):
    tp_idx = lax.axis_index("tp")
    return {"tp": LINE * (tp_idx // LINE) + lax.rem(lax.rem(tp_idx, LINE) + shift + LINE, LINE)}


def weight_gather(w_ref, all_ref, other_core, sends, recvs):
    core = lax.rem(lax.axis_index("cp"), 2)
    part_rows = w_ref.shape[0] // 2
    quarter = part_rows // 2
    first = core * part_rows

    def whole(slot):
        return all_ref.at[slot, pl.ds(first, part_rows)]

    def lo(slot):
        return all_ref.at[slot, pl.ds(first, quarter)]

    def hi(slot):
        return all_ref.at[slot, pl.ds(first + quarter, quarter)]

    own = w_ref.at[pl.ds(first, part_rows)]
    routes = [
        ("prev", own, whole(1), line_device(1)), ("next", own, whole(2), line_device(-1)),
        ("far_lo", lo(1), lo(3), line_device(1)), ("far_hi", hi(2), hi(3), line_device(-1)),
        ("prev_x", whole(1), whole(1), other_core), ("next_x", whole(2), whole(2), other_core),
        ("far_lo_x", lo(3), lo(3), other_core), ("far_hi_x", hi(3), hi(3), other_core),
    ]

    def copy_of(name):
        for idx, (kind, src, dst, target) in enumerate(routes):
            if kind == name:
                return pltpu.make_async_remote_copy(src_ref=src, dst_ref=dst, send_sem=sends.at[idx], recv_sem=recvs.at[idx],
                                                    device_id=target, device_id_type=pl.DeviceIdType.MESH)

    def start(*names):
        for name in names:
            copy_of(name).start()

    def wait_recv(*names):
        for name in names:
            copy_of(name).wait_recv()

    def wait_sends():
        for route in routes:
            copy_of(route[0]).wait_send()

    return start, wait_recv, wait_sends


def causal_mask(rows, cols, transposed=False):
    row_ids = lax.broadcasted_iota(jnp.int32, (rows, cols), 0)
    col_ids = lax.broadcasted_iota(jnp.int32, (rows, cols), 1)
    return col_ids >= row_ids if transposed else row_ids >= col_ids


def forward_kernel(n_sh, heads, dim, q_ref, kv_ref, wo_ref, o_ref, lse_ref, all_ref, wo_all_ref,
                   kv_buf, m_ref, l_ref, acc_ref, sends, recvs, w_sends, w_recvs, sems):
    rank, rank_of, barrier, start, wait_recv, wait_sends = shard_exchange(n_sh, [(kv_ref, kv_buf)], sends, recvs)
    n_x = n_sh // 2
    w_start, w_wait, w_wait_sends = weight_gather(wo_ref, wo_all_ref, {"cp": rank_of(0, 1)}, w_sends, w_recvs)
    barrier([line_device(1), line_device(-1)])
    start("prev", "next", "own_x")
    w_start("prev", "next")
    width = heads * dim
    half_rows = q_ref.shape[1]
    log2e_scale = math.log2(math.e) * dim ** -0.5
    own_w = pltpu.make_async_copy(wo_ref, wo_all_ref.at[0], sems.at[1])
    own_w.start()
    own = pltpu.make_async_copy(kv_ref, kv_buf.at[pl.ds(2 * rank, 2)], sems.at[0])
    own.start()
    own.wait()
    for half in range(2):
        for h in range(heads):
            cols = slice(h * dim, (h + 1) * dim)
            vcols = slice(width + h * dim, width + (h + 1) * dim)
            k_blk = kv_buf[2 * rank + half, :, cols]
            v_blk = kv_buf[2 * rank + half, :, vcols]
            s = dot_t(q_ref[half, :, cols], k_blk)
            s = jnp.where(causal_mask(half_rows, half_rows), s, -jnp.inf)
            m = jnp.max(s, axis=1, keepdims=True)
            p = jnp.exp2((s - m) * log2e_scale)
            m_ref[half, h] = jnp.broadcast_to(m, (half_rows, dim))
            l_ref[half, h] = jnp.broadcast_to(jnp.sum(p, axis=1, keepdims=True), (half_rows, dim))
            acc_ref[half, h] = dot_n(p.astype(BF16), v_blk)

    def unit(late, slot):
        for h in range(heads):
            cols = slice(h * dim, (h + 1) * dim)
            vcols = slice(width + h * dim, width + (h + 1) * dim)
            k_blk = kv_buf[slot, :, cols]
            v_blk = kv_buf[slot, :, vcols]
            s = dot_t(q_ref[late, :, cols], k_blk)
            m_old = m_ref[late, h]
            m_new = jnp.maximum(m_old, jnp.max(s, axis=1, keepdims=True))
            factor = jnp.exp2((m_old - m_new) * log2e_scale)
            p = jnp.exp2((s - m_new[:, :1]) * log2e_scale)
            m_ref[late, h] = m_new
            l_ref[late, h] = l_ref[late, h] * factor + jnp.sum(p, axis=1, keepdims=True)
            acc_ref[late, h] = acc_ref[late, h] * factor + dot_n(p.astype(BF16), v_blk)

    def visit(first, count, shard_of):
        def step(t, carry):
            shard = shard_of(t // 2)
            after = (shard > rank).astype(jnp.int32)
            second = lax.rem(t, 2)
            late = jnp.where(second == 1, after, 1)
            slot = 2 * shard + jnp.where(second == 1, after, 0)
            unit(late, slot)
            return carry
        lax.fori_loop(first, first + count, step, 0)

    offsets = [(0, 0), (0, 1), (n_x - 1, 0), (1, 0), (n_x - 1, 1), (1, 1), (2, 0), (2, 1)]

    def shard_of(idx):
        out = rank_of(*offsets[0])
        for pos in range(1, n_sh):
            out = jnp.where(idx == pos, rank_of(*offsets[pos]), out)
        return out

    visit(0, 1, shard_of)
    wait_recv("own_x")
    visit(2, 2, shard_of)
    wait_recv("prev")
    start("far_lo", "prev_x")
    wait_recv("next")
    start("far_hi", "next_x")
    visit(4, 4, shard_of)
    w_wait("prev")
    w_start("far_lo", "prev_x")
    w_wait("next")
    w_start("far_hi", "next_x")
    wait_recv("prev_x", "next_x")
    visit(8, 2, shard_of)
    wait_recv("far_lo", "far_hi")
    start("far_lo_x", "far_hi_x")
    visit(10, 4, shard_of)
    wait_recv("far_lo_x", "far_hi_x")
    out = pltpu.make_async_copy(kv_buf, all_ref, sems.at[0])
    out.start()
    visit(14, 2, shard_of)
    w_wait("far_lo", "far_hi")
    w_start("far_lo_x", "far_hi_x")
    for half in range(2):
        for h in range(heads):
            cols = slice(h * dim, (h + 1) * dim)
            l = l_ref[half, h]
            o_ref[half, :, cols] = (acc_ref[half, h] / l).astype(BF16)
            lse = m_ref[half, h] * log2e_scale + jnp.log2(l)
            lse_ref[half, h:h + 1, :] = jnp.transpose(lse)[:1]
    out.wait()
    own_w.wait()
    w_wait("prev_x", "next_x", "far_lo_x", "far_hi_x")
    wait_sends()
    w_wait_sends()


def stats_kernel(heads, dim, o_ref, do_ref, lse_ref, out_ref, rows_ref, o_buf, sends, recvs):
    y_pos = lax.rem(lax.axis_index("tp"), LINE)
    shifts = (0, 1, -1, 2)
    sem = pltpu.get_barrier_semaphore()
    for shift in shifts[1:]:
        pl.semaphore_signal(sem, inc=1, device_id=line_device(shift), device_id_type=pl.DeviceIdType.MESH)
    pl.semaphore_wait(sem, 3)
    copies = []
    for slot in range(1, LINE):
        target = line_device(shifts[slot])
        copies.append(pltpu.make_async_remote_copy(
            src_ref=o_ref.at[:, lax.rem(target["tp"], LINE)], dst_ref=o_buf.at[slot - 1], send_sem=sends.at[slot - 1],
            recv_sem=recvs.at[slot - 1], device_id=target, device_id_type=pl.DeviceIdType.MESH))
        copies[-1].start()
    width = heads * dim
    rows_ref[:, :, :width] = o_ref[:, y_pos]
    half_rows = lse_ref.shape[2]
    o_rows = o_ref[...].reshape(2, half_rows, width)
    for half in range(2):
        rows = [lse_ref[half]]
        for h in range(heads):
            cols = slice(h * dim, (h + 1) * dim)
            prod = do_ref[half, :, cols].astype(F32) * o_rows[half, :, cols].astype(F32)
            delta = jnp.broadcast_to(jnp.sum(prod, axis=1, keepdims=True), (half_rows, dim))
            rows.append(jnp.transpose(delta)[:1])
        rows.append(jnp.zeros((8 - 2 * heads, half_rows), F32))
        out_ref[half] = jnp.concatenate(rows, axis=0)
    for slot in range(1, LINE):
        copies[slot - 1].wait_recv()
        rows_ref[:, :, slot * width:(slot + 1) * width] = o_buf[slot - 1]
    for copy in copies:
        copy.wait_send()


def backward_kernel(n_sh, heads, dim, q_ref, do_ref, st_ref, all_ref, dq_ref, dkv_ref,
                    kv_buf, q_buf, do_buf, st_buf, acc_ref, lse_ref, dot_ref, dk_acc, dv_acc, sends, recvs, sems):
    rank, rank_of, barrier, start, wait_recv, wait_sends = shard_exchange(
        n_sh, [(q_ref, q_buf), (do_ref, do_buf), (st_ref, st_buf)], sends, recvs)
    n_x = n_sh // 2
    barrier()
    start("prev", "next", "own_x")
    load = [pltpu.make_async_copy(all_ref, kv_buf, sems.at[0])]
    for idx, (own, buf) in enumerate([(q_ref, q_buf), (do_ref, do_buf), (st_ref, st_buf)]):
        load.append(pltpu.make_async_copy(own, buf.at[pl.ds(2 * rank, 2)], sems.at[1 + idx]))
    for copy in load:
        copy.start()
    width = heads * dim
    half_rows = q_ref.shape[1]
    scale = dim ** -0.5
    log2e_scale = math.log2(math.e) * scale
    for half in range(2):
        for h in range(heads):
            lse_ref[half, h] = jnp.transpose(jnp.broadcast_to(st_ref[half, h:h + 1, :], (dim, half_rows)))
            dot_ref[half, h] = jnp.transpose(jnp.broadcast_to(st_ref[half, heads + h:heads + h + 1, :], (dim, half_rows)))
    for copy in load:
        copy.wait()

    def query_part(half, slot, h, masked):
        cols = slice(h * dim, (h + 1) * dim)
        vcols = slice(width + h * dim, width + (h + 1) * dim)
        k_blk = kv_buf[slot, :, cols]
        v_blk = kv_buf[slot, :, vcols]
        s = dot_t(q_ref[half, :, cols], k_blk)
        p = jnp.exp2(s * log2e_scale - lse_ref[half, h][:, :1])
        if masked:
            p = jnp.where(causal_mask(half_rows, half_rows), p, 0.0)
        dp = dot_t(do_ref[half, :, cols], v_blk)
        ds = (p * (dp - dot_ref[half, h][:, :1])).astype(BF16)
        return dot_n(ds, k_blk)

    for half in range(2):
        for h in range(heads):
            acc_ref[half, h] = query_part(half, 2 * rank + half, h, True)

    def query_step(t, carry):
        late = (t >= rank).astype(jnp.int32)
        slot = block_slot(t - late * rank, n_sh)
        for h in range(heads):
            acc_ref[late, h] = acc_ref[late, h] + query_part(late, slot, h, False)
        return carry

    lax.fori_loop(0, 2 * n_sh - 1, query_step, 0)
    wait_recv("prev")
    start("far_lo", "prev_x")
    wait_recv("next")
    start("far_hi", "next_x")
    for half in range(2):
        for h in range(heads):
            dq_ref[half, :, h * dim:(h + 1) * dim] = (acc_ref[half, h] * scale).astype(BF16)

    def key_part(half, slot, h, masked):
        cols = slice(h * dim, (h + 1) * dim)
        vcols = slice(width + h * dim, width + (h + 1) * dim)
        q_blk = q_buf[slot, :, cols]
        do_blk = do_buf[slot, :, cols]
        k_slot = 2 * rank + half
        s = dot_t(kv_buf[k_slot, :, cols], q_blk)
        p = jnp.exp2(s * log2e_scale - st_buf[slot, h:h + 1, :])
        if masked:
            p = jnp.where(causal_mask(half_rows, half_rows, transposed=True), p, 0.0)
        dp = dot_t(kv_buf[k_slot, :, vcols], do_blk)
        ds = (p * (dp - st_buf[slot, heads + h:heads + h + 1, :])).astype(BF16)
        return dot_n(ds, q_blk), dot_n(p.astype(BF16), do_blk)

    for half in range(2):
        for h in range(heads):
            dk_acc[half, h], dv_acc[half, h] = key_part(half, 2 * rank + half, h, True)

    offsets = [(0, 0), (0, 1), (n_x - 1, 0), (1, 0), (n_x - 1, 1), (1, 1), (2, 0), (2, 1)]

    def visit(first, count):
        def step(t, carry):
            idx = t // 2
            shard = rank_of(*offsets[0])
            for pos in range(1, n_sh):
                shard = jnp.where(idx == pos, rank_of(*offsets[pos]), shard)
            before = (shard < rank).astype(jnp.int32)
            second = lax.rem(t, 2)
            late = jnp.where(second == 1, before, 0)
            slot = 2 * shard + jnp.where(second == 1, before, 1)
            for h in range(heads):
                dk_part, dv_part = key_part(late, slot, h, False)
                dk_acc[late, h] = dk_acc[late, h] + dk_part
                dv_acc[late, h] = dv_acc[late, h] + dv_part
            return carry
        lax.fori_loop(first, first + count, step, 0)

    visit(0, 1)
    wait_recv("own_x")
    visit(2, 6)
    wait_recv("prev_x", "next_x")
    visit(8, 2)
    wait_recv("far_lo", "far_hi")
    start("far_lo_x", "far_hi_x")
    visit(10, 4)
    wait_recv("far_lo_x", "far_hi_x")
    visit(14, 2)
    for half in range(2):
        for h in range(heads):
            cols = slice(h * dim, (h + 1) * dim)
            vcols = slice(width + h * dim, width + (h + 1) * dim)
            dkv_ref[half, :, cols] = (dk_acc[half, h] * scale).astype(BF16)
            dkv_ref[half, :, vcols] = dv_acc[half, h].astype(BF16)
    wait_sends()


def gather_rows_kernel(x_ref, all_ref, sends, recvs, sem):
    tp_idx = lax.axis_index("tp")
    pos = (tp_idx // LINE, lax.rem(tp_idx, LINE))
    half_rows = x_ref.shape[0] // 2
    quarter = half_rows // 2

    def block(axis, fast, slow):
        off = (slow, fast) if axis == 1 else (fast, slow)
        z_idx, y_idx = [lax.rem(base + shift + LINE, LINE) for base, shift in zip(pos, off)]
        return LINE * z_idx + y_idx

    barrier = pltpu.get_barrier_semaphore()
    for axis in range(2):
        for shift in (1, -1):
            pl.semaphore_signal(barrier, inc=1, device_id={"tp": block(axis, shift, 0)}, device_id_type=pl.DeviceIdType.MESH)
    pl.semaphore_wait(barrier, 4)

    own = pltpu.make_async_copy(x_ref, all_ref.at[block(1, 0, 0)], sem.at[0])
    own.start()
    table = {}
    for colour in range(2):
        axis = 1 - colour
        base = colour * half_rows
        whole, low, high = (base, half_rows), (base, quarter), (base + quarter, quarter)

        def add(name, fast, slow, rows, along_fast, shift):
            idx = len(table)
            span = pl.ds(*rows)
            blk = block(axis, fast, slow)
            src = x_ref.at[span] if fast == 0 and slow == 0 else all_ref.at[blk, span]
            target = block(axis, shift, 0) if along_fast else block(axis, 0, shift)
            table[colour, name] = pltpu.make_async_remote_copy(
                src_ref=src, dst_ref=all_ref.at[blk, span], send_sem=sends.at[idx], recv_sem=recvs.at[idx],
                device_id={"tp": target}, device_id_type=pl.DeviceIdType.MESH)

        add("prev", 0, 0, whole, True, 1)
        add("next", 0, 0, whole, True, -1)
        add("far_lo", -1, 0, low, True, 1)
        add("far_hi", 1, 0, high, True, -1)
        for fast in (0, -1, 1, 2):
            add(("prev", fast), fast, 0, whole, False, 1)
            add(("next", fast), fast, 0, whole, False, -1)
            add(("far_lo", fast), fast, -1, low, False, 1)
            add(("far_hi", fast), fast, 1, high, False, -1)

    def start(*names):
        for name in names:
            for colour in range(2):
                table[colour, name].start()

    def wait(*names):
        for name in names:
            for colour in range(2):
                table[colour, name].wait_recv()

    start("prev", "next", ("prev", 0), ("next", 0))
    wait("prev")
    start("far_lo", ("prev", -1), ("next", -1))
    wait("next")
    start("far_hi", ("prev", 1), ("next", 1))
    wait(("prev", 0))
    start(("far_lo", 0))
    wait(("next", 0))
    start(("far_hi", 0))
    wait("far_lo", "far_hi")
    start(("prev", 2), ("next", 2))
    for fast in (-1, 1, 2):
        wait(("prev", fast))
        start(("far_lo", fast))
        wait(("next", fast))
        start(("far_hi", fast))
    for fast in (0, -1, 1, 2):
        wait(("far_lo", fast), ("far_hi", fast))
    own.wait()
    for copy in table.values():
        copy.wait_send()


def gather_rows(x_blk, n_tp):
    rows, cols = x_blk.shape
    if n_tp != LINE * LINE:
        return lax.all_gather(x_blk, "tp", axis=0, tiled=True)
    gathered = pl.pallas_call(
        gather_rows_kernel,
        name="gather_rows",
        out_shape=jax.ShapeDtypeStruct((n_tp, rows, cols), x_blk.dtype),
        in_specs=[VMEM_SPEC],
        out_specs=ANY_SPEC,
        scratch_shapes=[pltpu.SemaphoreType.DMA((40,)), pltpu.SemaphoreType.DMA((40,)), pltpu.SemaphoreType.DMA((1,))],
        compiler_params=pltpu.CompilerParams(collective_id=4, has_side_effects=True),
    )(x_blk)
    return gathered.reshape(n_tp * rows, cols)


VMEM_SPEC = pl.BlockSpec(memory_space=pltpu.VMEM)
ANY_SPEC = pl.BlockSpec(memory_space=pl.ANY)


def attention_call(kernel, name, collective_id, flops, in_specs, out_specs, out_shape, scratch):
    return pl.pallas_call(
        kernel,
        name=name,
        out_shape=out_shape,
        in_specs=in_specs,
        out_specs=out_specs,
        scratch_shapes=scratch,
        cost_estimate=pl.CostEstimate(flops=flops, bytes_accessed=10 * 2 ** 20, transcendentals=0),
        compiler_params=pltpu.CompilerParams(vmem_limit_bytes=VMEM_LIMIT, collective_id=collective_id, has_side_effects=True),
    )


def solution(mesh):
    n_sh = mesh.shape["cp"]

    def device_fn(x_blk, w_query, w_key, w_value, w_out, dy_blk):
        model_dim, heads, dim = w_query.shape
        width = heads * dim
        wq = w_query.reshape(model_dim, width)
        wkv = jnp.concatenate([w_key.reshape(model_dim, width), w_value.reshape(model_dim, width)], axis=1)
        wo = w_out.reshape(width, model_dim)

        x_rows = gather_rows(x_blk, mesh.shape["tp"])
        x_rows, dy_blk = lax.optimization_barrier((x_rows, dy_blk))
        dy_rows = lax.all_gather(dy_blk, "tp", axis=0, tiled=True)
        n_rows = x_rows.shape[0]
        half_rows = n_rows // 2
        tile_flops = 4 * (2 * n_sh + 1) * half_rows * half_rows * heads * dim

        kv = dot_n(x_rows, wkv).astype(BF16).reshape(2, half_rows, 2 * width)
        q = dot_n(x_rows, wq).astype(BF16).reshape(2, half_rows, width)
        acc = pltpu.VMEM((2, heads, half_rows, dim), F32)
        dma = pltpu.SemaphoreType.DMA
        kv_all_shape = (2 * n_sh, half_rows, 2 * width)

        o, lse, kv_all, wo_all = attention_call(
            functools.partial(forward_kernel, n_sh, heads, dim), "attn_fwd", 0, 2 * tile_flops,
            [VMEM_SPEC] * 3, [VMEM_SPEC, VMEM_SPEC, ANY_SPEC, ANY_SPEC],
            [jax.ShapeDtypeStruct((2, half_rows, width), BF16), jax.ShapeDtypeStruct((2, heads, half_rows), F32),
             jax.ShapeDtypeStruct(kv_all_shape, BF16), jax.ShapeDtypeStruct((LINE, width, model_dim), BF16)],
            [pltpu.VMEM(kv_all_shape, BF16), acc, acc, acc, dma((9,)), dma((9,)), dma((8,)), dma((8,)), dma((2,))],
        )(q, kv, wo)
        o_flat = o.reshape(n_rows, width)
        lse, *late_weights = lax.optimization_barrier((lse, w_query, w_key, w_value))
        w_all = jnp.concatenate([w_late.reshape(model_dim, width) for w_late in late_weights], axis=1)
        dy_rows, w_all = lax.optimization_barrier((dy_rows, w_all))
        d_o = dot_t(dy_rows, wo).astype(BF16).reshape(2, half_rows, width)
        n_z = mesh.shape["tp"] // LINE
        blk_rows = n_rows // mesh.shape["tp"]
        stats, o_rows = pl.pallas_call(
            functools.partial(stats_kernel, heads, dim),
            name="attn_stats",
            out_shape=[jax.ShapeDtypeStruct((2, 8, half_rows), F32), jax.ShapeDtypeStruct((n_z, blk_rows, LINE * width), BF16)],
            in_specs=[VMEM_SPEC] * 3,
            out_specs=[VMEM_SPEC] * 2,
            scratch_shapes=[pltpu.VMEM((LINE - 1, n_z, blk_rows, width), BF16), dma((LINE - 1,)), dma((LINE - 1,))],
            compiler_params=pltpu.CompilerParams(collective_id=2, has_side_effects=True),
        )(o.reshape(n_z, LINE, blk_rows, width), d_o, lse)
        y_part = dot_n(o_rows.reshape(n_z * blk_rows, LINE * width), wo_all.reshape(LINE * width, model_dim))
        y_part, stats = lax.optimization_barrier((y_part, stats))
        columns = [[LINE * z_idx + y_idx for z_idx in range(n_z)] for y_idx in range(LINE)]
        y_blk = lax.psum_scatter(y_part, "tp", scatter_dimension=0, axis_index_groups=columns, tiled=True).astype(BF16)
        shard_buf = pltpu.VMEM((2 * n_sh, half_rows, width), BF16)
        dq, dkv = attention_call(
            functools.partial(backward_kernel, n_sh, heads, dim), "attn_bwd", 1, 7 * tile_flops // 2,
            [VMEM_SPEC, VMEM_SPEC, VMEM_SPEC, ANY_SPEC], [VMEM_SPEC, VMEM_SPEC],
            [jax.ShapeDtypeStruct((2, half_rows, width), BF16), jax.ShapeDtypeStruct((2, half_rows, 2 * width), BF16)],
            [pltpu.VMEM(kv_all_shape, BF16), shard_buf, shard_buf, pltpu.VMEM((2 * n_sh, 8, half_rows), F32),
             acc, acc, acc, acc, acc, dma((27,)), dma((27,)), dma((4,))],
        )(q, d_o, stats, kv_all)

        dq_flat = dq.reshape(n_rows, width)
        dkv_flat = dkv.reshape(n_rows, 2 * width)
        d_all = jnp.concatenate([dq_flat, dkv_flat], axis=1)
        dx_part = dot_t(d_all, w_all)
        dx_blk = lax.psum_scatter(dx_part, "tp", scatter_dimension=0, tiled=True).astype(BF16)

        def weight_grad(lhs, rhs, shape):
            return lax.dot_general(lhs, rhs, ROWS_CONTRACT, preferred_element_type=F32).astype(BF16).reshape(shape)[None]

        grad_wo = weight_grad(o_flat, dy_rows, (heads, dim, model_dim))
        grad_wq = weight_grad(x_rows, dq_flat, (model_dim, heads, dim))
        grad_wk = weight_grad(x_rows, dkv_flat[:, :width], (model_dim, heads, dim))
        grad_wv = weight_grad(x_rows, dkv_flat[:, width:], (model_dim, heads, dim))
        return y_blk, dx_blk, grad_wq, grad_wk, grad_wv, grad_wo

    return jax.shard_map(device_fn, mesh=mesh,
                         in_specs=(ROW_SPEC, HEAD_SPEC, HEAD_SPEC, HEAD_SPEC, OUT_W_SPEC, ROW_SPEC),
                         out_specs=(ROW_SPEC, ROW_SPEC, GRAD_SPEC, GRAD_SPEC, GRAD_SPEC, GRAD_OUT_SPEC),
                         check_vma=False)
```

```python
import functools
import math

import jax
import jax.numpy as jnp
from jax import lax
from jax.experimental import pallas as pl
from jax.experimental.pallas import tpu as pltpu
from jax.sharding import PartitionSpec as P

ROW_SPEC = P(("dp", "cp", "tp"), None)
HEAD_SPEC = P(None, "tp", None)
OUT_W_SPEC = P("tp", None, None)
GRAD_SPEC = P(("dp", "cp"), None, "tp", None)
GRAD_OUT_SPEC = P(("dp", "cp"), "tp", None, None)
COLS_CONTRACT = (((1,), (1,)), ((), ()))
ROWS_CONTRACT = (((0,), (0,)), ((), ()))
VMEM_LIMIT = 58 * 1024 * 1024
F32 = jnp.float32
BF16 = jnp.bfloat16


def dot_t(lhs, rhs):
    return lax.dot_general(lhs, rhs, COLS_CONTRACT, preferred_element_type=F32)


def dot_n(lhs, rhs):
    return jnp.dot(lhs, rhs, preferred_element_type=F32)


LINE = 4


def block_slot(pos_blk, n_sh):
    return jnp.where(pos_blk < n_sh, 2 * pos_blk, 2 * (2 * n_sh - 1 - pos_blk) + 1)


def shard_exchange(n_sh, pairs, sends, recvs):
    n_x = n_sh // 2
    rank = lax.axis_index("cp")
    chip, core = rank // 2, lax.rem(rank, 2)

    def rank_of(dx, dc):
        return 2 * lax.rem(chip + dx, n_x) + lax.rem(core + dc, 2)

    n_kinds = 9
    kinds = {"prev": 0, "next": 1, "far_lo": 2, "far_hi": 3, "own_x": 4, "prev_x": 5, "next_x": 6, "far_lo_x": 7, "far_hi_x": 8}

    def part(buf, dx, dc, half):
        return buf.at[pl.ds(2 * rank_of(dx, dc) + (0 if half is None else half), 2 if half is None else 1)]

    routes = {
        "prev": ((0, 0), None, (1, 0)), "next": ((0, 0), None, (n_x - 1, 0)), "own_x": ((0, 0), None, (0, 1)),
        "far_lo": ((n_x - 1, 0), 0, (1, 0)), "far_hi": ((1, 0), 1, (n_x - 1, 0)),
        "prev_x": ((n_x - 1, 0), None, (0, 1)), "next_x": ((1, 0), None, (0, 1)),
        "far_lo_x": ((2, 0), 0, (0, 1)), "far_hi_x": ((2, 0), 1, (0, 1)),
    }

    def copies(kind):
        (dx, dc), half, target = routes[kind]
        out = []
        for idx, (own, buf) in enumerate(pairs):
            dst = part(buf, dx, dc, half)
            src = own if (dx, dc) == (0, 0) else dst
            out.append(pltpu.make_async_remote_copy(
                src_ref=src, dst_ref=dst, send_sem=sends.at[idx * n_kinds + kinds[kind]], recv_sem=recvs.at[idx * n_kinds + kinds[kind]],
                device_id={"cp": rank_of(*target)}, device_id_type=pl.DeviceIdType.MESH))
        return out

    def start(*names):
        for name in names:
            for copy in copies(name):
                copy.start()

    def wait_recv(*names):
        for name in names:
            for copy in copies(name):
                copy.wait_recv()

    def wait_sends():
        for name in routes:
            for copy in copies(name):
                copy.wait_send()

    def barrier(others=()):
        sem = pltpu.get_barrier_semaphore()
        for target in [{"cp": rank_of(*offset)} for offset in ((1, 0), (n_x - 1, 0), (0, 1))] + list(others):
            pl.semaphore_signal(sem, inc=1, device_id=target, device_id_type=pl.DeviceIdType.MESH)
        pl.semaphore_wait(sem, 3 + len(others))

    return rank, rank_of, barrier, start, wait_recv, wait_sends


def line_device(shift):
    tp_idx = lax.axis_index("tp")
    return {"tp": LINE * (tp_idx // LINE) + lax.rem(lax.rem(tp_idx, LINE) + shift + LINE, LINE)}


def weight_gather(w_ref, all_ref, other_core, sends, recvs):
    core = lax.rem(lax.axis_index("cp"), 2)
    part_rows = w_ref.shape[0] // 2
    quarter = part_rows // 2
    first = core * part_rows

    def whole(slot):
        return all_ref.at[slot, pl.ds(first, part_rows)]

    def lo(slot):
        return all_ref.at[slot, pl.ds(first, quarter)]

    def hi(slot):
        return all_ref.at[slot, pl.ds(first + quarter, quarter)]

    own = w_ref.at[pl.ds(first, part_rows)]
    routes = [
        ("prev", own, whole(1), line_device(1)), ("next", own, whole(2), line_device(-1)),
        ("far_lo", lo(1), lo(3), line_device(1)), ("far_hi", hi(2), hi(3), line_device(-1)),
        ("prev_x", whole(1), whole(1), other_core), ("next_x", whole(2), whole(2), other_core),
        ("far_lo_x", lo(3), lo(3), other_core), ("far_hi_x", hi(3), hi(3), other_core),
    ]

    def copy_of(name):
        for idx, (kind, src, dst, target) in enumerate(routes):
            if kind == name:
                return pltpu.make_async_remote_copy(src_ref=src, dst_ref=dst, send_sem=sends.at[idx], recv_sem=recvs.at[idx],
                                                    device_id=target, device_id_type=pl.DeviceIdType.MESH)

    def start(*names):
        for name in names:
            copy_of(name).start()

    def wait_recv(*names):
        for name in names:
            copy_of(name).wait_recv()

    def wait_sends():
        for route in routes:
            copy_of(route[0]).wait_send()

    return start, wait_recv, wait_sends


def causal_mask(rows, cols, transposed=False):
    row_ids = lax.broadcasted_iota(jnp.int32, (rows, cols), 0)
    col_ids = lax.broadcasted_iota(jnp.int32, (rows, cols), 1)
    return col_ids >= row_ids if transposed else row_ids >= col_ids


def forward_kernel(n_sh, heads, dim, q_ref, kv_ref, wo_ref, o_ref, lse_ref, all_ref, wo_all_ref,
                   kv_buf, m_ref, l_ref, acc_ref, sends, recvs, w_sends, w_recvs, sems):
    rank, rank_of, barrier, start, wait_recv, wait_sends = shard_exchange(n_sh, [(kv_ref, kv_buf)], sends, recvs)
    n_x = n_sh // 2
    w_start, w_wait, w_wait_sends = weight_gather(wo_ref, wo_all_ref, {"cp": rank_of(0, 1)}, w_sends, w_recvs)
    barrier([line_device(1), line_device(-1)])
    start("prev", "next", "own_x")
    w_start("prev", "next")
    width = heads * dim
    half_rows = q_ref.shape[1]
    log2e_scale = math.log2(math.e) * dim ** -0.5
    own_w = pltpu.make_async_copy(wo_ref, wo_all_ref.at[0], sems.at[1])
    own_w.start()
    own = pltpu.make_async_copy(kv_ref, kv_buf.at[pl.ds(2 * rank, 2)], sems.at[0])
    own.start()
    own.wait()

    def diagonal(half, carry):
        for h in range(heads):
            cols = slice(h * dim, (h + 1) * dim)
            vcols = slice(width + h * dim, width + (h + 1) * dim)
            k_blk = kv_buf[2 * rank + half, :, cols]
            v_blk = kv_buf[2 * rank + half, :, vcols]
            s = dot_t(q_ref[half, :, cols], k_blk)
            s = jnp.where(causal_mask(half_rows, half_rows), s, -jnp.inf)
            m = jnp.max(s, axis=1, keepdims=True)
            p = jnp.exp2((s - m) * log2e_scale)
            m_ref[half, h] = jnp.broadcast_to(m, (half_rows, dim))
            l_ref[half, h] = jnp.broadcast_to(jnp.sum(p, axis=1, keepdims=True), (half_rows, dim))
            acc_ref[half, h] = dot_n(p.astype(BF16), v_blk)
        return carry

    lax.fori_loop(0, 2, diagonal, 0)

    def unit(late, slot):
        for h in range(heads):
            cols = slice(h * dim, (h + 1) * dim)
            vcols = slice(width + h * dim, width + (h + 1) * dim)
            k_blk = kv_buf[slot, :, cols]
            v_blk = kv_buf[slot, :, vcols]
            s = dot_t(q_ref[late, :, cols], k_blk)
            m_old = m_ref[late, h]
            m_new = jnp.maximum(m_old, jnp.max(s, axis=1, keepdims=True))
            factor = jnp.exp2((m_old - m_new) * log2e_scale)
            p = jnp.exp2((s - m_new[:, :1]) * log2e_scale)
            m_ref[late, h] = m_new
            l_ref[late, h] = l_ref[late, h] * factor + jnp.sum(p, axis=1, keepdims=True)
            acc_ref[late, h] = acc_ref[late, h] * factor + dot_n(p.astype(BF16), v_blk)

    def visit_all(count, shard_of, actions):
        def step(u, carry):
            for pos, action in actions.items():
                pl.when(u == pos)(action)
            t = u + (u > 0).astype(jnp.int32)
            shard = shard_of(t // 2)
            after = (shard > rank).astype(jnp.int32)
            second = lax.rem(t, 2)
            late = jnp.where(second == 1, after, 1)
            slot = 2 * shard + jnp.where(second == 1, after, 0)
            unit(late, slot)
            return carry
        lax.fori_loop(0, count, step, 0)

    offsets = [(0, 0), (0, 1), (n_x - 1, 0), (1, 0), (n_x - 1, 1), (1, 1), (2, 0), (2, 1)]

    def shard_of(idx):
        out = rank_of(*offsets[0])
        for pos in range(1, n_sh):
            out = jnp.where(idx == pos, rank_of(*offsets[pos]), out)
        return out

    out = pltpu.make_async_copy(kv_buf, all_ref, sems.at[0])

    def take_near():
        wait_recv("prev")
        start("far_lo", "prev_x")
        wait_recv("next")
        start("far_hi", "next_x")

    def take_near_other():
        w_wait("prev")
        w_start("far_lo", "prev_x")
        w_wait("next")
        w_start("far_hi", "next_x")
        wait_recv("prev_x", "next_x")

    def take_far():
        wait_recv("far_lo", "far_hi")
        start("far_lo_x", "far_hi_x")

    def take_far_other():
        wait_recv("far_lo_x", "far_hi_x")
        out.start()

    visit_all(2 * n_sh - 1, shard_of, {1: lambda: wait_recv("own_x"), 3: take_near, 7: take_near_other, 9: take_far, 13: take_far_other})
    w_wait("far_lo", "far_hi")
    w_start("far_lo_x", "far_hi_x")

    def finish(half, carry):
        for h in range(heads):
            cols = slice(h * dim, (h + 1) * dim)
            l = l_ref[half, h]
            o_ref[half, :, cols] = (acc_ref[half, h] / l).astype(BF16)
            lse = m_ref[half, h] * log2e_scale + jnp.log2(l)
            lse_ref[half, h:h + 1, :] = jnp.transpose(lse)[:1]
        return carry

    lax.fori_loop(0, 2, finish, 0)
    out.wait()
    own_w.wait()
    w_wait("prev_x", "next_x", "far_lo_x", "far_hi_x")
    wait_sends()
    w_wait_sends()


def stats_kernel(heads, dim, o_ref, do_ref, lse_ref, out_ref, rows_ref, o_buf, sends, recvs):
    y_pos = lax.rem(lax.axis_index("tp"), LINE)
    shifts = (0, 1, -1, 2)
    sem = pltpu.get_barrier_semaphore()
    for shift in shifts[1:]:
        pl.semaphore_signal(sem, inc=1, device_id=line_device(shift), device_id_type=pl.DeviceIdType.MESH)
    pl.semaphore_wait(sem, 3)
    copies = []
    for slot in range(1, LINE):
        target = line_device(shifts[slot])
        copies.append(pltpu.make_async_remote_copy(
            src_ref=o_ref.at[:, lax.rem(target["tp"], LINE)], dst_ref=o_buf.at[slot - 1], send_sem=sends.at[slot - 1],
            recv_sem=recvs.at[slot - 1], device_id=target, device_id_type=pl.DeviceIdType.MESH))
        copies[-1].start()
    width = heads * dim
    rows_ref[:, :, :width] = o_ref[:, y_pos]
    half_rows = lse_ref.shape[2]
    o_rows = o_ref[...].reshape(2, half_rows, width)
    for half in range(2):
        rows = [lse_ref[half]]
        for h in range(heads):
            cols = slice(h * dim, (h + 1) * dim)
            prod = do_ref[half, :, cols].astype(F32) * o_rows[half, :, cols].astype(F32)
            delta = jnp.broadcast_to(jnp.sum(prod, axis=1, keepdims=True), (half_rows, dim))
            rows.append(jnp.transpose(delta)[:1])
        rows.append(jnp.zeros((8 - 2 * heads, half_rows), F32))
        out_ref[half] = jnp.concatenate(rows, axis=0)
    for slot in range(1, LINE):
        copies[slot - 1].wait_recv()
        rows_ref[:, :, slot * width:(slot + 1) * width] = o_buf[slot - 1]
    for copy in copies:
        copy.wait_send()


def backward_kernel(n_sh, heads, dim, q_ref, do_ref, st_ref, all_ref, dq_ref, dkv_ref,
                    kv_buf, q_buf, do_buf, st_buf, acc_ref, lse_ref, dot_ref, dk_acc, dv_acc, sends, recvs, sems):
    rank, rank_of, barrier, start, wait_recv, wait_sends = shard_exchange(
        n_sh, [(q_ref, q_buf), (do_ref, do_buf), (st_ref, st_buf)], sends, recvs)
    n_x = n_sh // 2
    barrier()
    start("prev", "next", "own_x")
    load = [pltpu.make_async_copy(all_ref, kv_buf, sems.at[0])]
    for idx, (own, buf) in enumerate([(q_ref, q_buf), (do_ref, do_buf), (st_ref, st_buf)]):
        load.append(pltpu.make_async_copy(own, buf.at[pl.ds(2 * rank, 2)], sems.at[1 + idx]))
    for copy in load:
        copy.start()
    width = heads * dim
    half_rows = q_ref.shape[1]
    scale = dim ** -0.5
    log2e_scale = math.log2(math.e) * scale

    def spread(half, carry):
        for h in range(heads):
            lse_ref[half, h] = jnp.transpose(jnp.broadcast_to(st_ref[half, h:h + 1, :], (dim, half_rows)))
            dot_ref[half, h] = jnp.transpose(jnp.broadcast_to(st_ref[half, heads + h:heads + h + 1, :], (dim, half_rows)))
        return carry

    lax.fori_loop(0, 2, spread, 0)
    for copy in load:
        copy.wait()

    def query_part(half, slot, h, masked):
        cols = slice(h * dim, (h + 1) * dim)
        vcols = slice(width + h * dim, width + (h + 1) * dim)
        k_blk = kv_buf[slot, :, cols]
        v_blk = kv_buf[slot, :, vcols]
        s = dot_t(q_ref[half, :, cols], k_blk)
        p = jnp.exp2(s * log2e_scale - lse_ref[half, h][:, :1])
        if masked:
            p = jnp.where(causal_mask(half_rows, half_rows), p, 0.0)
        dp = dot_t(do_ref[half, :, cols], v_blk)
        ds = (p * (dp - dot_ref[half, h][:, :1])).astype(BF16)
        return dot_n(ds, k_blk)

    def query_diagonal(half, carry):
        for h in range(heads):
            acc_ref[half, h] = query_part(half, 2 * rank + half, h, True)
        return carry

    lax.fori_loop(0, 2, query_diagonal, 0)

    def query_step(t, carry):
        late = (t >= rank).astype(jnp.int32)
        slot = block_slot(t - late * rank, n_sh)
        for h in range(heads):
            acc_ref[late, h] = acc_ref[late, h] + query_part(late, slot, h, False)
        return carry

    lax.fori_loop(0, 2 * n_sh - 1, query_step, 0)
    wait_recv("prev")
    start("far_lo", "prev_x")
    wait_recv("next")
    start("far_hi", "next_x")
    for half in range(2):
        for h in range(heads):
            dq_ref[half, :, h * dim:(h + 1) * dim] = (acc_ref[half, h] * scale).astype(BF16)

    def key_part(half, slot, h, masked):
        cols = slice(h * dim, (h + 1) * dim)
        vcols = slice(width + h * dim, width + (h + 1) * dim)
        q_blk = q_buf[slot, :, cols]
        do_blk = do_buf[slot, :, cols]
        k_slot = 2 * rank + half
        s = dot_t(kv_buf[k_slot, :, cols], q_blk)
        p = jnp.exp2(s * log2e_scale - st_buf[slot, h:h + 1, :])
        if masked:
            p = jnp.where(causal_mask(half_rows, half_rows, transposed=True), p, 0.0)
        dp = dot_t(kv_buf[k_slot, :, vcols], do_blk)
        ds = (p * (dp - st_buf[slot, heads + h:heads + h + 1, :])).astype(BF16)
        return dot_n(ds, q_blk), dot_n(p.astype(BF16), do_blk)

    def key_diagonal(half, carry):
        for h in range(heads):
            dk_acc[half, h], dv_acc[half, h] = key_part(half, 2 * rank + half, h, True)
        return carry

    lax.fori_loop(0, 2, key_diagonal, 0)

    offsets = [(0, 0), (0, 1), (n_x - 1, 0), (1, 0), (n_x - 1, 1), (1, 1), (2, 0), (2, 1)]

    def visit_all(count, actions):
        def step(u, carry):
            for at_step, action in actions.items():
                pl.when(u == at_step)(action)
            t = u + (u > 0).astype(jnp.int32)
            idx = t // 2
            shard = rank_of(*offsets[0])
            for pos in range(1, n_sh):
                shard = jnp.where(idx == pos, rank_of(*offsets[pos]), shard)
            before = (shard < rank).astype(jnp.int32)
            second = lax.rem(t, 2)
            late = jnp.where(second == 1, before, 0)
            slot = 2 * shard + jnp.where(second == 1, before, 1)
            for h in range(heads):
                dk_part, dv_part = key_part(late, slot, h, False)
                dk_acc[late, h] = dk_acc[late, h] + dk_part
                dv_acc[late, h] = dv_acc[late, h] + dv_part
            return carry
        lax.fori_loop(0, count, step, 0)

    def take_far():
        wait_recv("far_lo", "far_hi")
        start("far_lo_x", "far_hi_x")

    visit_all(2 * n_sh - 1, {1: lambda: wait_recv("own_x"), 7: lambda: wait_recv("prev_x", "next_x"), 9: take_far,
                             13: lambda: wait_recv("far_lo_x", "far_hi_x")})
    for half in range(2):
        for h in range(heads):
            cols = slice(h * dim, (h + 1) * dim)
            vcols = slice(width + h * dim, width + (h + 1) * dim)
            dkv_ref[half, :, cols] = (dk_acc[half, h] * scale).astype(BF16)
            dkv_ref[half, :, vcols] = dv_acc[half, h].astype(BF16)
    wait_sends()


def gather_rows_kernel(x_ref, all_ref, sends, recvs, sem):
    tp_idx = lax.axis_index("tp")
    pos = (tp_idx // LINE, lax.rem(tp_idx, LINE))
    half_rows = x_ref.shape[0] // 2
    quarter = half_rows // 2

    def block(axis, fast, slow):
        off = (slow, fast) if axis == 1 else (fast, slow)
        z_idx, y_idx = [lax.rem(base + shift + LINE, LINE) for base, shift in zip(pos, off)]
        return LINE * z_idx + y_idx

    barrier = pltpu.get_barrier_semaphore()
    for axis in range(2):
        for shift in (1, -1):
            pl.semaphore_signal(barrier, inc=1, device_id={"tp": block(axis, shift, 0)}, device_id_type=pl.DeviceIdType.MESH)
    pl.semaphore_wait(barrier, 4)

    own = pltpu.make_async_copy(x_ref, all_ref.at[block(1, 0, 0)], sem.at[0])
    own.start()
    table = {}
    for colour in range(2):
        axis = 1 - colour
        base = colour * half_rows
        whole, low, high = (base, half_rows), (base, quarter), (base + quarter, quarter)

        def add(name, fast, slow, rows, along_fast, shift):
            idx = len(table)
            span = pl.ds(*rows)
            blk = block(axis, fast, slow)
            src = x_ref.at[span] if fast == 0 and slow == 0 else all_ref.at[blk, span]
            target = block(axis, shift, 0) if along_fast else block(axis, 0, shift)
            table[colour, name] = pltpu.make_async_remote_copy(
                src_ref=src, dst_ref=all_ref.at[blk, span], send_sem=sends.at[idx], recv_sem=recvs.at[idx],
                device_id={"tp": target}, device_id_type=pl.DeviceIdType.MESH)

        add("prev", 0, 0, whole, True, 1)
        add("next", 0, 0, whole, True, -1)
        add("far_lo", -1, 0, low, True, 1)
        add("far_hi", 1, 0, high, True, -1)
        for fast in (0, -1, 1, 2):
            add(("prev", fast), fast, 0, whole, False, 1)
            add(("next", fast), fast, 0, whole, False, -1)
            add(("far_lo", fast), fast, -1, low, False, 1)
            add(("far_hi", fast), fast, 1, high, False, -1)

    def start(*names):
        for name in names:
            for colour in range(2):
                table[colour, name].start()

    def wait(*names):
        for name in names:
            for colour in range(2):
                table[colour, name].wait_recv()

    start("prev", "next", ("prev", 0), ("next", 0))
    wait("prev")
    start("far_lo", ("prev", -1), ("next", -1))
    wait("next")
    start("far_hi", ("prev", 1), ("next", 1))
    wait(("prev", 0))
    start(("far_lo", 0))
    wait(("next", 0))
    start(("far_hi", 0))
    wait("far_lo", "far_hi")
    start(("prev", 2), ("next", 2))
    for fast in (-1, 1, 2):
        wait(("prev", fast))
        start(("far_lo", fast))
        wait(("next", fast))
        start(("far_hi", fast))
    for fast in (0, -1, 1, 2):
        wait(("far_lo", fast), ("far_hi", fast))
    own.wait()
    for copy in table.values():
        copy.wait_send()


def gather_rows(x_blk, n_tp):
    rows, cols = x_blk.shape
    if n_tp != LINE * LINE:
        return lax.all_gather(x_blk, "tp", axis=0, tiled=True)
    gathered = pl.pallas_call(
        gather_rows_kernel,
        name="gather_rows",
        out_shape=jax.ShapeDtypeStruct((n_tp, rows, cols), x_blk.dtype),
        in_specs=[VMEM_SPEC],
        out_specs=ANY_SPEC,
        scratch_shapes=[pltpu.SemaphoreType.DMA((40,)), pltpu.SemaphoreType.DMA((40,)), pltpu.SemaphoreType.DMA((1,))],
        compiler_params=pltpu.CompilerParams(collective_id=4, has_side_effects=True),
    )(x_blk)
    return gathered.reshape(n_tp * rows, cols)


VMEM_SPEC = pl.BlockSpec(memory_space=pltpu.VMEM)
ANY_SPEC = pl.BlockSpec(memory_space=pl.ANY)


def attention_call(kernel, name, collective_id, flops, in_specs, out_specs, out_shape, scratch):
    return pl.pallas_call(
        kernel,
        name=name,
        out_shape=out_shape,
        in_specs=in_specs,
        out_specs=out_specs,
        scratch_shapes=scratch,
        cost_estimate=pl.CostEstimate(flops=flops, bytes_accessed=10 * 2 ** 20, transcendentals=0),
        compiler_params=pltpu.CompilerParams(vmem_limit_bytes=VMEM_LIMIT, collective_id=collective_id, has_side_effects=True),
    )


def solution(mesh):
    n_sh = mesh.shape["cp"]

    def device_fn(x_blk, w_query, w_key, w_value, w_out, dy_blk):
        model_dim, heads, dim = w_query.shape
        width = heads * dim
        wq = w_query.reshape(model_dim, width)
        wkv = jnp.concatenate([w_key.reshape(model_dim, width), w_value.reshape(model_dim, width)], axis=1)
        wo = w_out.reshape(width, model_dim)

        x_rows = gather_rows(x_blk, mesh.shape["tp"])
        x_rows, dy_blk = lax.optimization_barrier((x_rows, dy_blk))
        dy_rows = lax.all_gather(dy_blk, "tp", axis=0, tiled=True)
        n_rows = x_rows.shape[0]
        half_rows = n_rows // 2
        tile_flops = 4 * (2 * n_sh + 1) * half_rows * half_rows * heads * dim

        kv = dot_n(x_rows, wkv).astype(BF16).reshape(2, half_rows, 2 * width)
        q = dot_n(x_rows, wq).astype(BF16).reshape(2, half_rows, width)
        acc = pltpu.VMEM((2, heads, half_rows, dim), F32)
        dma = pltpu.SemaphoreType.DMA
        kv_all_shape = (2 * n_sh, half_rows, 2 * width)

        o, lse, kv_all, wo_all = attention_call(
            functools.partial(forward_kernel, n_sh, heads, dim), "attn_fwd", 0, 2 * tile_flops,
            [VMEM_SPEC] * 3, [VMEM_SPEC, VMEM_SPEC, ANY_SPEC, ANY_SPEC],
            [jax.ShapeDtypeStruct((2, half_rows, width), BF16), jax.ShapeDtypeStruct((2, heads, half_rows), F32),
             jax.ShapeDtypeStruct(kv_all_shape, BF16), jax.ShapeDtypeStruct((LINE, width, model_dim), BF16)],
            [pltpu.VMEM(kv_all_shape, BF16), acc, acc, acc, dma((9,)), dma((9,)), dma((8,)), dma((8,)), dma((2,))],
        )(q, kv, wo)
        o_flat = o.reshape(n_rows, width)
        lse, *late_weights = lax.optimization_barrier((lse, w_query, w_key, w_value))
        w_all = jnp.concatenate([w_late.reshape(model_dim, width) for w_late in late_weights], axis=1)
        dy_rows, w_all = lax.optimization_barrier((dy_rows, w_all))
        d_o = dot_t(dy_rows, wo).astype(BF16).reshape(2, half_rows, width)
        n_z = mesh.shape["tp"] // LINE
        blk_rows = n_rows // mesh.shape["tp"]
        stats, o_rows = pl.pallas_call(
            functools.partial(stats_kernel, heads, dim),
            name="attn_stats",
            out_shape=[jax.ShapeDtypeStruct((2, 8, half_rows), F32), jax.ShapeDtypeStruct((n_z, blk_rows, LINE * width), BF16)],
            in_specs=[VMEM_SPEC] * 3,
            out_specs=[VMEM_SPEC] * 2,
            scratch_shapes=[pltpu.VMEM((LINE - 1, n_z, blk_rows, width), BF16), dma((LINE - 1,)), dma((LINE - 1,))],
            compiler_params=pltpu.CompilerParams(collective_id=2, has_side_effects=True),
        )(o.reshape(n_z, LINE, blk_rows, width), d_o, lse)
        y_part = dot_n(o_rows.reshape(n_z * blk_rows, LINE * width), wo_all.reshape(LINE * width, model_dim))
        y_part, stats = lax.optimization_barrier((y_part, stats))
        columns = [[LINE * z_idx + y_idx for z_idx in range(n_z)] for y_idx in range(LINE)]
        y_blk = lax.psum_scatter(y_part, "tp", scatter_dimension=0, axis_index_groups=columns, tiled=True).astype(BF16)
        shard_buf = pltpu.VMEM((2 * n_sh, half_rows, width), BF16)
        dq, dkv = attention_call(
            functools.partial(backward_kernel, n_sh, heads, dim), "attn_bwd", 1, 7 * tile_flops // 2,
            [VMEM_SPEC, VMEM_SPEC, VMEM_SPEC, ANY_SPEC], [VMEM_SPEC, VMEM_SPEC],
            [jax.ShapeDtypeStruct((2, half_rows, width), BF16), jax.ShapeDtypeStruct((2, half_rows, 2 * width), BF16)],
            [pltpu.VMEM(kv_all_shape, BF16), shard_buf, shard_buf, pltpu.VMEM((2 * n_sh, 8, half_rows), F32),
             acc, acc, acc, acc, acc, dma((27,)), dma((27,)), dma((4,))],
        )(q, d_o, stats, kv_all)

        dq_flat = dq.reshape(n_rows, width)
        dkv_flat = dkv.reshape(n_rows, 2 * width)
        d_all = jnp.concatenate([dq_flat, dkv_flat], axis=1)
        dx_part = dot_t(d_all, w_all)
        dx_blk = lax.psum_scatter(dx_part, "tp", scatter_dimension=0, tiled=True).astype(BF16)

        def weight_grad(lhs, rhs, shape):
            return lax.dot_general(lhs, rhs, ROWS_CONTRACT, preferred_element_type=F32).astype(BF16).reshape(shape)[None]

        grad_wo = weight_grad(o_flat, dy_rows, (heads, dim, model_dim))
        grad_wq = weight_grad(x_rows, dq_flat, (model_dim, heads, dim))
        grad_wk = weight_grad(x_rows, dkv_flat[:, :width], (model_dim, heads, dim))
        grad_wv = weight_grad(x_rows, dkv_flat[:, width:], (model_dim, heads, dim))
        return y_blk, dx_blk, grad_wq, grad_wk, grad_wv, grad_wo

    return jax.shard_map(device_fn, mesh=mesh,
                         in_specs=(ROW_SPEC, HEAD_SPEC, HEAD_SPEC, HEAD_SPEC, OUT_W_SPEC, ROW_SPEC),
                         out_specs=(ROW_SPEC, ROW_SPEC, GRAD_SPEC, GRAD_SPEC, GRAD_SPEC, GRAD_OUT_SPEC),
                         check_vma=False)
```
